512 devices in a mesh: sx: 32 (over z, core), sy: 16 (over x, y).
Axes of the slice: x: 4, y: 4, z: 16, core: 2. Of those that a mesh axis runs over, the one named last changes fastest.
Arguments:
- features: bfloat16 [64, 512, 2048], P(None, 'sx', 'sy'), may hold values from -6 to 6
- enc_weight: bfloat16 [3, 3, 3, 64, 64], replicated, may hold values from -0.15625 to 0.15625
- enc_bias: float32 [64], replicated, may hold values from -3 to 3
- proj_weight: bfloat16 [64, 512], replicated, may hold values from -0.25 to 0.25
- bottle_weight: bfloat16 [3, 3, 3, 512, 512], P(None, None, None, 'sy'), may hold values from -0.0546875 to 0.0546875
- bottle_bias: float32 [512], P('sy'), may hold values from -3 to 3
- out_weight: bfloat16 [512, 64], P('sy'), may hold values from -0.25 to 0.25
- dec_weight: bfloat16 [3, 3, 3, 64, 64], replicated, may hold values from -0.15625 to 0.15625
- dec_bias: float32 [64], replicated, may hold values from -3 to 3
Outputs:
- decoded: bfloat16 [64, 512, 2048], P(None, 'sx', 'sy')
The draws below stay inside these ranges and needn't reach their ends.
All inputs are finite; a program needn't handle non-finite values.
Results may differ from the reference program's by a relative error of at most 0.009.
Values may be sent and summed in bfloat16 or wider, within the bound.
No kernel may reach another device: no remote copies, remote signals or barrier semaphores. Data moves between devices by JAX's collectives and lax.ppermute only.
A program may use at most 64 MiB of HBM per device.

```python
import jax
import jax.numpy as jnp
from jax import lax

C = 64
CB = 512
POOL = 8
FZ = 16
NX = 512
NY = 128


def steps_of(rng, extent, split, smallest, high):
    loudness = 1.0
    for dim, shards_of in split:
        heights = jax.random.uniform(jax.random.fold_in(jax.random.fold_in(rng, 6), dim), (shards_of,), jnp.float32, smallest / len(split), high / len(split))
        loudness = loudness * jnp.repeat(jnp.exp(heights), extent[dim] // shards_of).reshape((-1,) + (1,) * (len(extent) - 1 - dim))
    return loudness


def scatter_about(stream_key, extent, deviation, reach, split=(), held_as=jnp.bfloat16):
    factor_of = steps_of(stream_key, extent, split, -0.22, 0.18) if split else 1.0
    array = jax.random.normal(stream_key, extent, jnp.float32) * deviation * factor_of
    return jnp.minimum(jnp.maximum(array, -reach), reach).astype(held_as)


def setup_inputs(seed: int = 0) -> dict:
    splits = jax.random.split(jax.random.key(seed), 10)
    return {
        "features": scatter_about(splits[0], (C, NX, NY * FZ), 1.0, 6.0, ((1, 32), (2, 16))),
        "enc_weight": scatter_about(splits[1], (3, 3, 3, C, C), (27 * C) ** -0.5, 0.15625),
        "enc_bias": scatter_about(splits[2], (C,), 0.5, 3.0, (), jnp.float32),
        "proj_weight": scatter_about(splits[3], (C, CB), (9 * C) ** -0.5, 0.25),
        "bottle_weight": scatter_about(splits[4], (3, 3, 3, CB, CB), (27 * CB) ** -0.5, 0.0546875, ((3, 16),)),
        "bottle_bias": scatter_about(splits[5], (CB,), 0.5, 3.0, ((0, 16),), jnp.float32),
        "out_weight": scatter_about(splits[6], (CB, C), CB ** -0.5, 0.25, ((0, 16),)),
        "dec_weight": scatter_about(splits[7], (3, 3, 3, C, C), (27 * C) ** -0.5, 0.15625),
        "dec_bias": scatter_about(splits[8], (C,), 0.5, 3.0, (), jnp.float32),
    }


layout = ("NCDHW", "DHWOI", "NCDHW")


def convolve(field, kernel):
    result = lax.conv_general_dilated(field[None].astype(jnp.float32), kernel.astype(jnp.float32), (1, 1, 1), ((1, 1), (1, 1), (1, 1)), dimension_numbers=layout, precision=lax.Precision.HIGHEST)
    return result[0]


def interpolate(fine_count, fine_first, coarse_count, coarse_first, coarse_total):
    fine_index = fine_first + jnp.arange(fine_count, dtype=jnp.int32)
    coarse_index = coarse_first + jnp.arange(coarse_count, dtype=jnp.int32)
    numerator = 2 * fine_index + 1 - POOL
    low_cell = jnp.floor_divide(numerator, 2 * POOL)
    weight_high = (numerator - 2 * POOL * low_cell).astype(jnp.float32) / jnp.float32(2 * POOL)
    weight_high = jnp.where(low_cell < 0, jnp.float32(0.0), weight_high)
    low_cell = jnp.maximum(low_cell, 0)
    weight_high = jnp.where(low_cell >= coarse_total - 1, jnp.float32(0.0), weight_high)
    low_cell = jnp.minimum(low_cell, coarse_total - 1)
    low_hit = (coarse_index[None, :] == low_cell[:, None]).astype(jnp.float32)
    high_hit = (coarse_index[None, :] == low_cell[:, None] + 1).astype(jnp.float32)
    return (1.0 - weight_high)[:, None] * low_hit + weight_high[:, None] * high_hit


def reference(features, enc_weight, enc_bias, proj_weight, bottle_weight, bottle_bias, out_weight, dec_weight, dec_bias):
    highest = lax.Precision.HIGHEST
    channels, size_x, merged = features.shape
    size_z = FZ
    size_y = merged // size_z
    field = features.reshape(channels, size_x, size_y, size_z)
    encoded = jax.nn.relu(convolve(field, enc_weight) + enc_bias[:, None, None, None]).astype(jnp.bfloat16)
    cells_x, cells_y, cells_z = size_x // POOL, size_y // POOL, size_z // POOL
    pooled = jnp.max(encoded.reshape(channels, cells_x, POOL, cells_y, POOL, cells_z, POOL), axis=(2, 4, 6))
    projected = jnp.einsum("ck,cxyz->kxyz", proj_weight.astype(jnp.float32), pooled.astype(jnp.float32), precision=highest).astype(jnp.bfloat16)
    bottleneck = jax.nn.relu(convolve(projected, bottle_weight) + bottle_bias[:, None, None, None]).astype(jnp.bfloat16)
    lowres = jnp.einsum("kc,kxyz->cxyz", out_weight.astype(jnp.float32), bottleneck.astype(jnp.float32), precision=highest)
    along_x = interpolate(size_x, 0, cells_x, 0, cells_x)
    along_y = interpolate(size_y, 0, cells_y, 0, cells_y)
    along_z = interpolate(size_z, 0, cells_z, 0, cells_z)
    step_one = jnp.einsum("kabc,zc->kabz", lowres, along_z, precision=highest)
    step_two = jnp.einsum("kabz,yb->kayz", step_one, along_y, precision=highest)
    upsampled = jnp.einsum("kayz,xa->kxyz", step_two, along_x, precision=highest)
    joined = (encoded.astype(jnp.float32) + upsampled).astype(jnp.bfloat16)
    decoded = (convolve(joined, dec_weight) + dec_bias[:, None, None, None]).astype(jnp.bfloat16)
    return decoded.reshape(channels, size_x, merged)
```

```python
import jax
import jax.numpy as jnp
from jax import lax
from jax.experimental import pallas as pl
from jax.experimental.pallas import tpu as pltpu
from jax.sharding import PartitionSpec as P

F32 = jnp.float32
BF = jnp.bfloat16
C = 64
NSX = 32
NSY = 16
VM = pl.BlockSpec(memory_space=pltpu.VMEM)


def call(kernel, outs, *ins, name, scratch=(), flops=1000000, limit=16):
    return pl.pallas_call(
        kernel,
        out_shape=outs,
        in_specs=[VM] * len(ins),
        out_specs=jax.tree.map(lambda _: VM, outs),
        scratch_shapes=list(scratch),
        name=name,
        compiler_params=pltpu.CompilerParams(vmem_limit_bytes=limit * 2**20),
        cost_estimate=pl.CostEstimate(flops=flops, transcendentals=0, bytes_accessed=100000),
    )(*ins)


def S(shape, dtype):
    return jax.ShapeDtypeStruct(shape, dtype)


def dot(a, b):
    return jnp.dot(a, b, preferred_element_type=F32)


def dot_nt(a, b):
    return lax.dot_general(a, b, (((1,), (1,)), ((), ())), preferred_element_type=F32)


def lanes_of(rows):
    return lax.broadcasted_iota(jnp.int32, (rows, 128), 1)


def roll(v, shift):
    shift = shift % 128
    return v if shift == 0 else pltpu.roll(v, shift, 1)


def k_features(x_ref, ft_ref, lo_ref, hi_ref, buf):
    buf[...] = x_ref[...].reshape(C * 16, 128).astype(F32)
    for x in range(16):
        row = buf[pl.ds(x, C, stride=16), :].astype(BF)
        ft_ref[x] = row
        if x < 2:
            lo_ref[x] = row
        if x >= 14:
            hi_ref[x - 14] = row


def row_of(r, lo_ref, ft_ref, hi_ref):
    if r < 2:
        return lo_ref[r]
    if r < 18:
        return ft_ref[r - 2]
    return hi_ref[r - 18]


def k_faces(lo_ref, ft_ref, hi_ref, left_ref, right_ref):
    lane = lanes_of(C)
    for g in range(5):
        left = None
        for q in range(4):
            row = row_of(4 * g + q, lo_ref, ft_ref, hi_ref).astype(F32)
            a, b = roll(row, 32 * q), roll(row, 32 * q - 96)
            if q == 0:
                left, right = a, b
            else:
                here = lane >= 32 * q
                left, right = jnp.where(here, a, left), jnp.where(here, b, right)
        left_ref[g] = left.astype(BF)
        right_ref[g] = right.astype(BF)


def arranged(w_ref, out_ref):
    for a in range(3):
        for pair in range(5):
            blocks = [w_ref[a * 9 + t] for t in range(2 * pair, min(2 * pair + 2, 9))]
            wide = blocks[0] if len(blocks) == 1 else jnp.concatenate(blocks, axis=1)
            out_ref[pl.ds(a * C, C), pl.ds(128 * pair, wide.shape[1])] = wide


def column(b_ref):
    row = jnp.broadcast_to(b_ref[...], (C, C))
    same = lax.broadcasted_iota(jnp.int32, (C, C), 0) == lax.broadcasted_iota(jnp.int32, (C, C), 1)
    return jnp.broadcast_to(jnp.sum(jnp.where(same, row, 0.0), axis=1, keepdims=True), (C, 128))


def k_enc_weights(w_ref, b_ref, out_ref, bias_ref):
    arranged(w_ref, out_ref)
    bias_ref[...] = column(b_ref)


def interp_weight(g, cell, count, cells):
    num = 2 * g - 7
    low = jnp.right_shift(num, 4)
    w = (num - 16 * low).astype(F32) * (1.0 / 16.0)
    w = jnp.where((low < 0) | (low >= cells - 1), 0.0, w)
    low = jnp.clip(low, 0, cells - 1)
    value = jnp.where(cell == low, 1.0 - w, jnp.where(cell == low + 1, w, 0.0))
    return jnp.where((g >= 0) & (g < count), value, 0.0)


def k_dec_weights(w_ref, b_ref, bw_ref, proj_ref, ow_ref, bb_ref, out_ref, bias_ref, vt_ref, ow2_ref, bb2_ref, s_ref):
    arranged(w_ref, out_ref)
    bias_ref[...] = column(b_ref)
    proj = proj_ref[...]
    r = dot_nt(bw_ref[...], jnp.concatenate([proj, proj], axis=0))
    half = lanes_of(C) < C
    for ab in range(9):
        both = jnp.where(half, r[96 * ab : 96 * ab + 64], r[96 * ab + 32 : 96 * ab + 96])
        vt_ref[:, pl.ds(128 * ab, 128)] = both.astype(BF)
    ow = ow_ref[...]
    none = jnp.zeros_like(ow)
    ow2_ref[...] = jnp.concatenate(
        [jnp.concatenate([ow, none], axis=1), jnp.concatenate([none, ow], axis=1)], axis=0
    )
    bb2_ref[...] = jnp.concatenate([bb_ref[...], bb_ref[...]], axis=1)
    j = lax.axis_index("sy")
    row = lax.broadcasted_iota(jnp.int32, (32, 128), 0)
    lane = lax.broadcasted_iota(jnp.int32, (32, 128), 1)
    y, z = jnp.right_shift(lane, 4), jnp.bitwise_and(lane, 15)
    cell_y = j - 1 + jnp.right_shift(row, 3)
    zero = jnp.zeros((96, 128), BF)
    for b in range(3):
        wy = interp_weight(8 * j + y + (b - 1), cell_y, 8 * NSY, NSY)
        wy = jnp.where(row < 24, wy, 0.0)
        for c in range(3):
            for zo in range(2):
                wz = interp_weight(z + (c - 1), 1 - zo, 16, 2)
                at = pl.ds(128 * (3 * b + c), 128)
                s_ref[pl.ds(128 * zo, 32), at] = (wy * wz).astype(BF)
                s_ref[pl.ds(128 * zo + 32, 96), at] = zero


def z_taps(v, out_ref, b, at, z):
    k = 3 * C * b
    out_ref[pl.ds(k, C), at] = jnp.where(z == 0, 0.0, roll(v, 1)).astype(BF)
    out_ref[pl.ds(k + C, C), at] = v.astype(BF)
    out_ref[pl.ds(k + 2 * C, C), at] = jnp.where(z == 15, 0.0, roll(v, -1)).astype(BF)


def y_taps(own, left, left_at, right, right_at, out_ref, at, lane, z):
    z_taps(roll(jnp.where(lane >= 112, roll(left, 112 - left_at), own), 16), out_ref, 0, at, z)
    z_taps(own, out_ref, 1, at, z)
    z_taps(roll(jnp.where(lane < 16, roll(right, -right_at), own), -16), out_ref, 2, at, z)


def k_encode(
    lo_ref, ft_ref, hi_ref, fl_ref, fr_ref, hl_ref, hr_ref, w_ref, bias_ref, em_ref, eh_ref, pool_ref, xm, g_ref
):
    lane = lanes_of(C)
    z = jnp.bitwise_and(lane, 15)
    even = jnp.bitwise_and(lane, 16) == 0
    s, j = lax.axis_index("sx"), lax.axis_index("sy")
    for g in range(5):
        hl, hr = hl_ref[g].astype(F32), hr_ref[g].astype(F32)
        fl, fr = fl_ref[g].astype(F32), fr_ref[g].astype(F32)
        for q in range(4):
            r = 4 * g + q
            own = row_of(r, lo_ref, ft_ref, hi_ref).astype(F32)
            y_taps(own, hl, 32 * q + 16, hr, 32 * q, xm, pl.ds(128 * r, 128), lane, z)
        at = pl.ds(128 * (20 + g), 128)
        z_taps(jnp.where(even, hl, fr), xm, 0, at, z)
        z_taps(jnp.where(even, roll(hl, -16), roll(hr, 16)), xm, 1, at, z)
        z_taps(jnp.where(even, fl, hr), xm, 2, at, z)
    w = w_ref[...]
    for n in range(0, 25, 5):
        g_ref[:, pl.ds(128 * n, 640)] = dot(w, xm[:, pl.ds(128 * n, 640)])
    bias = bias_ref[...]
    best = [None, None]
    for r in range(18):
        v = g_ref[pl.ds(0, C), pl.ds(128 * r, 128)] + g_ref[pl.ds(C, C), pl.ds(128 * (r + 1), 128)]
        v = v + g_ref[pl.ds(2 * C, C), pl.ds(128 * (r + 2), 128)] + bias
        v = jnp.maximum(v, 0.0)
        if r == 0:
            v = jnp.where(s == 0, 0.0, v)
        if r == 17:
            v = jnp.where(s == NSX - 1, 0.0, v)
        v = v.astype(BF)
        em_ref[r] = v
        if 1 <= r <= 16:
            cell = (r - 1) // 8
            v = v.astype(F32)
            best[cell] = v if best[cell] is None else jnp.maximum(best[cell], v)
    outside = (even & (j == 0)) | (~even & (j == NSY - 1))
    for g in range(5):
        v = g_ref[pl.ds(0, C), pl.ds(128 * (20 + g), 128)] + bias
        for a in (1, 2):
            this = g_ref[pl.ds(a * C, C), pl.ds(128 * (20 + g), 128)]
            after = g_ref[pl.ds(a * C, C), pl.ds(128 * (20 + min(g + 1, 4)), 128)]
            v = v + roll(jnp.where(lane < 32 * a, after, this), -32 * a)
        v = jnp.where(outside, 0.0, jnp.maximum(v, 0.0))
        if g == 0:
            v = jnp.where((lane < 32) & (s == 0), 0.0, v)
        if g == 4:
            v = jnp.where((lane >= 64) | ((lane >= 32) & (s == NSX - 1)), 0.0, v)
        eh_ref[g] = v.astype(BF)
    for cell in range(2):
        m = best[cell]
        for shift in (64, 32, 16, -1, -2, -4):
            m = jnp.maximum(m, roll(m, shift))
        best[cell] = m
    first = lane == 0
    both = [jnp.where(first, best[0], roll(best[1], 1)), jnp.where(first, roll(best[0], -8), roll(best[1], -7))]
    pool_ref[...] = jnp.transpose(jnp.concatenate(both, axis=0))[:8]


def k_decode(em_ref, eh_ref, w_ref, bias_ref, d_ref, xm, g_ref):
    lane = lanes_of(C)
    z = jnp.bitwise_and(lane, 15)
    for r in range(18):
        own = em_ref[r].astype(F32)
        eh = eh_ref[r // 4].astype(F32)
        q = r % 4
        y_taps(own, eh, 32 * q, eh, 32 * q + 16, xm, pl.ds(128 * r, 128), lane, z)
    w = w_ref[...]
    for n in range(0, 18, 6):
        g_ref[:, pl.ds(128 * n, 768)] = dot(w, xm[:, pl.ds(128 * n, 768)])
    bias = bias_ref[...]
    for x in range(16):
        v = g_ref[pl.ds(0, C), pl.ds(128 * x, 128)] + g_ref[pl.ds(C, C), pl.ds(128 * (x + 1), 128)]
        d_ref[x] = v + g_ref[pl.ds(2 * C, C), pl.ds(128 * (x + 2), 128)] + bias


def k_message(left_ref, own_ref, right_ref, out_ref):
    message = jnp.concatenate(
        [left_ref[0:2], own_ref[0:2], right_ref[0:2], jnp.zeros((2, 128), F32)], axis=0
    )
    for i in range(NSY):
        out_ref[i] = message


def k_bottleneck(p_ref, vt_ref, bb_ref, ow_ref, out_ref):
    p = p_ref[...]
    pieces = []
    none = jnp.zeros((1, 8, 128), F32)
    for a in range(3):
        moved = p if a == 0 else jnp.concatenate([p[:, a:], p[:, :a]], axis=1)
        for b in range(3):
            if b == 0:
                v = jnp.concatenate([none, moved[:-1]], axis=0)
            elif b == 1:
                v = moved
            else:
                v = jnp.concatenate([moved[1:], none], axis=0)
            pieces.append(v.reshape(128, 128).astype(BF))
    h = dot_nt(jnp.concatenate(pieces, axis=1), vt_ref[...])
    h = jnp.maximum(h + bb_ref[...], 0.0).astype(BF)
    low = dot(h, ow_ref[...]).astype(BF).astype(F32)
    zero = jnp.zeros((8, 128), F32)
    for i in range(NSY):
        before = low[8 * (i - 1) : 8 * i] if i else zero
        after = low[8 * (i + 1) : 8 * (i + 2)] if i < NSY - 1 else zero
        out_ref[i] = jnp.concatenate([before, low[8 * i : 8 * i + 8], after], axis=0).astype(BF)


def k_final(parts_ref, s_ref, w_ref, d_ref, out_ref, xt, q_ref, buf):
    total = parts_ref[0].astype(F32)
    for i in range(1, NSY):
        total = total + parts_ref[i].astype(F32)
    total = jnp.concatenate([total, jnp.zeros((104, 128), F32)], axis=0)
    lt = jnp.transpose(total)
    lane = lanes_of(C)
    left = []
    for cell in range(4):
        here = jnp.bitwise_and(lane, 7) == cell
        left.append(jnp.concatenate([jnp.where(here, lt[:C], 0.0), jnp.where(here, lt[C:], 0.0)], axis=1).astype(BF))
    t = dot(jnp.concatenate(left, axis=0), s_ref[...])
    for cell in range(4):
        for bc in range(9):
            xt[pl.ds(C * bc, C), pl.ds(128 * cell, 128)] = t[
                C * cell : C * cell + C, 128 * bc : 128 * bc + 128
            ].astype(BF)
    q_ref[...] = dot(w_ref[...], xt[...])
    s = lax.axis_index("sx")
    for x in range(16):
        v = d_ref[x]
        for a in range(3):
            g = x + a - 1
            num = 2 * g - 7
            low = num // 16
            high = (num - 16 * low) / 16.0
            cell = low + 1
            w_low, w_high = jnp.float32(1.0 - high), jnp.float32(high)
            first, last = s == 0, s == NSX - 1
            if cell == 0:
                w_low = jnp.where(first, 0.0, w_low)
                w_high = jnp.where(first, 0.0 if g < 0 else 1.0, w_high)
            if cell == 2:
                w_low = jnp.where(last, 0.0 if g > 15 else 1.0, w_low)
                w_high = jnp.where(last, 0.0, w_high)
            v = v + w_low * q_ref[pl.ds(C * a, C), pl.ds(128 * cell, 128)]
            v = v + w_high * q_ref[pl.ds(C * a, C), pl.ds(128 * (cell + 1), 128)]
        buf[pl.ds(x, C, stride=16), :] = v
    out_ref[...] = buf[...].reshape(C, 16, 128).astype(BF)


def shifted(v, axis, step):
    size = lax.axis_size(axis)
    return lax.ppermute(v, axis, [(i, i + step) for i in range(size) if 0 <= i + step < size])


def per_device(features, enc_weight, enc_bias, proj_weight, bottle_weight, bottle_bias, out_weight, dec_weight, dec_bias):
    ft, lo, hi = call(
        k_features,
        (S((16, C, 128), BF), S((2, C, 128), BF), S((2, C, 128), BF)),
        features,
        name="features",
        scratch=[pltpu.VMEM((C * 16, 128), F32)],
    )
    x_lo, x_hi = shifted(hi, "sx", 1), shifted(lo, "sx", -1)
    we, be = call(
        k_enc_weights,
        (S((3 * C, 9 * C), BF), S((C, 128), F32)),
        enc_weight.reshape(27, C, C),
        enc_bias.reshape(1, C),
        name="enc_weights",
        flops=10**8,
    )
    fl, fr = call(k_faces, (S((5, C, 128), BF), S((5, C, 128), BF)), x_lo, ft, x_hi, name="faces")
    hl, hr = shifted(fr, "sy", 1), shifted(fl, "sy", -1)
    wd, bd, vt, ow2, bb2, smat = call(
        k_dec_weights,
        (
            S((3 * C, 9 * C), BF),
            S((C, 128), F32),
            S((C, 9 * 128), BF),
            S((C, 128), BF),
            S((1, C), F32),
            S((256, 9 * 128), BF),
        ),
        dec_weight.reshape(27, C, C),
        dec_bias.reshape(1, C),
        bottle_weight.reshape(27 * 32, 512),
        proj_weight,
        out_weight,
        bottle_bias.reshape(1, 32),
        name="dec_weights",
        flops=4 * 10**8,
    )
    em, eh, pooled = call(
        k_encode,
        (S((18, C, 128), BF), S((5, C, 128), BF), S((8, 128), F32)),
        x_lo,
        ft,
        x_hi,
        fl,
        fr,
        hl,
        hr,
        we,
        be,
        name="encode",
        scratch=[pltpu.VMEM((9 * C, 25 * 128), BF), pltpu.VMEM((3 * C, 25 * 128), F32)],
    )
    p_lo, p_hi = shifted(pooled, "sx", 1), shifted(pooled, "sx", -1)
    d = call(
        k_decode,
        S((16, C, 128), F32),
        em,
        eh,
        wd,
        bd,
        name="decode",
        scratch=[pltpu.VMEM((9 * C, 18 * 128), BF), pltpu.VMEM((3 * C, 18 * 128), F32)],
        flops=4 * 10**8,
    )
    message = call(k_message, S((NSY, 8, 128), F32), p_lo, pooled, p_hi, name="message")
    everyone = lax.all_to_all(message, "sy", 0, 0, tiled=True)
    partial = call(k_bottleneck, S((NSY, 24, 128), BF), everyone, vt, bb2, ow2, name="bottleneck")
    parts = lax.all_to_all(partial, "sy", 0, 0, tiled=True)
    return call(
        k_final,
        S((C, 16, 128), BF),
        parts,
        smat,
        wd,
        d,
        name="final",
        scratch=[
            pltpu.VMEM((9 * C, 512), BF),
            pltpu.VMEM((3 * C, 512), F32),
            pltpu.VMEM((C * 16, 128), F32),
        ],
    )


def solution(mesh):
    in_specs = (P(None, "sx", "sy"), P(), P(), P(), P(None, None, None, "sy", None), P("sy"), P("sy", None), P(), P())
    return jax.shard_map(per_device, mesh=mesh, in_specs=in_specs, out_specs=P(None, "sx", "sy"), check_vma=False)
```

```python
import jax
import jax.numpy as jnp
from jax import lax
from jax.experimental import pallas as pl
from jax.experimental.pallas import tpu as pltpu
from jax.sharding import PartitionSpec as P

F32 = jnp.float32
BF = jnp.bfloat16
C = 64
NSX = 32
NSY = 16
VM = pl.BlockSpec(memory_space=pltpu.VMEM)


def call(kernel, outs, *ins, name, scratch=(), flops=1000000, limit=16):
    return pl.pallas_call(
        kernel,
        out_shape=outs,
        in_specs=[VM] * len(ins),
        out_specs=jax.tree.map(lambda _: VM, outs),
        scratch_shapes=list(scratch),
        name=name,
        compiler_params=pltpu.CompilerParams(vmem_limit_bytes=limit * 2**20),
        cost_estimate=pl.CostEstimate(flops=flops, transcendentals=0, bytes_accessed=100000),
    )(*ins)


def S(shape, dtype):
    return jax.ShapeDtypeStruct(shape, dtype)


def dot(a, b):
    return jnp.dot(a, b, preferred_element_type=F32)


def dot_nt(a, b):
    return lax.dot_general(a, b, (((1,), (1,)), ((), ())), preferred_element_type=F32)


def lanes_of(rows):
    return lax.broadcasted_iota(jnp.int32, (rows, 128), 1)


def roll(v, shift):
    shift = shift % 128
    return v if shift == 0 else pltpu.roll(v, shift, 1)


def even_of(axis):
    return lax.rem(lax.axis_index(axis), 2) == 0


def k_features(x_ref, ft_ref, inner_ref, outer_ref, buf):
    buf[...] = x_ref[...].reshape(C * 16, 128).astype(F32)
    even = even_of("sx")

    def row(x):
        return buf[pl.ds(x, C, stride=16), :]

    for k in range(2):
        low, high = row(k), row(14 + k)
        inner_ref[k] = jnp.where(even, high, low).astype(BF)
        outer_ref[k] = jnp.where(even, low, high).astype(BF)
    for x in range(16):
        ft_ref[x + 2] = row(x).astype(BF)


def k_faces(inner_ref, outer_ref, ft_ref, x_ref, left_ref, right_ref, s_inner_ref, s_outer_ref):
    lane = lanes_of(C)
    even_x, even_y = even_of("sx"), even_of("sy")
    for k in range(2):
        inner, outer = inner_ref[k], outer_ref[k]
        x_ref[k] = jnp.where(even_x, outer, inner)
        x_ref[2 + k] = jnp.where(even_x, inner, outer)
    for g in range(5):
        left = None
        for q in range(4):
            r = 4 * g + q
            v = x_ref[r] if r < 2 else ft_ref[r] if r < 18 else x_ref[r - 16]
            v = v.astype(F32)
            a, b = roll(v, 32 * q), roll(v, 32 * q - 96)
            if q == 0:
                left, right = a, b
            else:
                here = lane >= 32 * q
                left, right = jnp.where(here, a, left), jnp.where(here, b, right)
        left_ref[g] = left.astype(BF)
        right_ref[g] = right.astype(BF)
        s_inner_ref[g] = jnp.where(even_y, right, left).astype(BF)
        s_outer_ref[g] = jnp.where(even_y, left, right).astype(BF)


def arranged(w_ref, out_ref):
    for a in range(3):
        for pair in range(5):
            blocks = [w_ref[a * 9 + t] for t in range(2 * pair, min(2 * pair + 2, 9))]
            wide = blocks[0] if len(blocks) == 1 else jnp.concatenate(blocks, axis=1)
            out_ref[pl.ds(a * C, C), pl.ds(128 * pair, wide.shape[1])] = wide


def column(b_ref):
    row = jnp.broadcast_to(b_ref[...], (C, C))
    same = lax.broadcasted_iota(jnp.int32, (C, C), 0) == lax.broadcasted_iota(jnp.int32, (C, C), 1)
    return jnp.broadcast_to(jnp.sum(jnp.where(same, row, 0.0), axis=1, keepdims=True), (C, 128))


def k_enc_weights(w_ref, b_ref, out_ref, bias_ref):
    arranged(w_ref, out_ref)
    bias_ref[...] = column(b_ref)


def interp_weight(g, cell, count, cells):
    num = 2 * g - 7
    low = jnp.right_shift(num, 4)
    w = (num - 16 * low).astype(F32) * (1.0 / 16.0)
    w = jnp.where((low < 0) | (low >= cells - 1), 0.0, w)
    low = jnp.clip(low, 0, cells - 1)
    value = jnp.where(cell == low, 1.0 - w, jnp.where(cell == low + 1, w, 0.0))
    return jnp.where((g >= 0) & (g < count), value, 0.0)


def k_dec_weights(w_ref, b_ref, bw_ref, proj_ref, ow_ref, bb_ref, out_ref, bias_ref, vt_ref, ow2_ref, bb2_ref, s_ref):
    arranged(w_ref, out_ref)
    bias_ref[...] = column(b_ref)
    proj = proj_ref[...]
    r = dot_nt(bw_ref[...], jnp.concatenate([proj, proj], axis=0))
    half = lanes_of(C) < C
    for ab in range(9):
        both = jnp.where(half, r[96 * ab : 96 * ab + 64], r[96 * ab + 32 : 96 * ab + 96])
        vt_ref[:, pl.ds(128 * ab, 128)] = both.astype(BF)
    ow = ow_ref[...]
    none = jnp.zeros_like(ow)
    ow2_ref[...] = jnp.concatenate(
        [jnp.concatenate([ow, none], axis=1), jnp.concatenate([none, ow], axis=1)], axis=0
    )
    bb2_ref[...] = jnp.concatenate([bb_ref[...], bb_ref[...]], axis=1)
    j = lax.axis_index("sy")
    row = lax.broadcasted_iota(jnp.int32, (32, 128), 0)
    lane = lax.broadcasted_iota(jnp.int32, (32, 128), 1)
    y, z = jnp.right_shift(lane, 4), jnp.bitwise_and(lane, 15)
    cell_y = j - 1 + jnp.right_shift(row, 3)
    zero = jnp.zeros((96, 128), BF)
    for b in range(3):
        wy = interp_weight(8 * j + y + (b - 1), cell_y, 8 * NSY, NSY)
        wy = jnp.where(row < 24, wy, 0.0)
        for c in range(3):
            for zo in range(2):
                wz = interp_weight(z + (c - 1), 1 - zo, 16, 2)
                at = pl.ds(128 * (3 * b + c), 128)
                s_ref[pl.ds(128 * zo, 32), at] = (wy * wz).astype(BF)
                s_ref[pl.ds(128 * zo + 32, 96), at] = zero


def z_taps(v, out_ref, b, at, z):
    k = 3 * C * b
    zero = jnp.zeros_like(v)
    out_ref[at, pl.ds(k, C), :] = jnp.where(z == 0, zero, roll(v, 1))
    out_ref[at, pl.ds(k + C, C), :] = v
    out_ref[at, pl.ds(k + 2 * C, C), :] = jnp.where(z == 15, zero, roll(v, -1))


def y_taps(own, left, left_at, right, right_at, out_ref, at, lane, z):
    z_taps(roll(jnp.where(lane >= 112, roll(left, 112 - left_at), own), 16), out_ref, 0, at, z)
    z_taps(own, out_ref, 1, at, z)
    z_taps(roll(jnp.where(lane < 16, roll(right, -right_at), own), -16), out_ref, 2, at, z)


def products(w_ref, xm, g_ref, first, last):
    w = w_ref[...]
    for n in range(first, last, 2):
        if n + 1 < last:
            g = dot(w, jnp.concatenate([xm[n], xm[n + 1]], axis=1))
            g_ref[n] = g[:, :128]
            g_ref[n + 1] = g[:, 128:]
        else:
            g_ref[n] = dot(w, xm[n])


def k_encode(
    ft_ref, x_ref, fl_ref, fr_ref, inner_ref, outer_ref, w_ref, bias_ref, em_ref, eh_ref, pool_ref, xm, g_ref
):
    lane = lanes_of(C)
    z = jnp.bitwise_and(lane, 15)
    even = jnp.bitwise_and(lane, 16) == 0
    s, j = lax.axis_index("sx"), lax.axis_index("sy")
    even_y = even_of("sy")
    for g in range(5):
        inner, outer = inner_ref[g], outer_ref[g]
        hl, hr = jnp.where(even_y, outer, inner), jnp.where(even_y, inner, outer)
        fl, fr = fl_ref[g], fr_ref[g]
        for q in range(4):
            r = 4 * g + q
            own = x_ref[r] if r < 2 else ft_ref[r] if r < 18 else x_ref[r - 16]
            y_taps(own, hl, 32 * q + 16, hr, 32 * q, xm, r, lane, z)
        at = 20 + g
        z_taps(jnp.where(even, hl, fr), xm, 0, at, z)
        z_taps(jnp.where(even, roll(hl, -16), roll(hr, 16)), xm, 1, at, z)
        z_taps(jnp.where(even, fl, hr), xm, 2, at, z)
    products(w_ref, xm, g_ref, 0, 25)
    bias = bias_ref[...]
    best = [None, None]
    for r in range(18):
        v = g_ref[r, pl.ds(0, C), :] + g_ref[r + 1, pl.ds(C, C), :] + g_ref[r + 2, pl.ds(2 * C, C), :] + bias
        v = jnp.maximum(v, 0.0)
        if r == 0:
            v = jnp.where(s == 0, 0.0, v)
        if r == 17:
            v = jnp.where(s == NSX - 1, 0.0, v)
        em_ref[r] = v.astype(BF)
        if 1 <= r <= 16:
            cell = (r - 1) // 8
            best[cell] = v if best[cell] is None else jnp.maximum(best[cell], v)
    outside = (even & (j == 0)) | (~even & (j == NSY - 1))
    for g in range(5):
        v = g_ref[20 + g, pl.ds(0, C), :] + bias
        for a in (1, 2):
            this = g_ref[20 + g, pl.ds(a * C, C), :]
            after = g_ref[20 + min(g + 1, 4), pl.ds(a * C, C), :]
            v = v + roll(jnp.where(lane < 32 * a, after, this), -32 * a)
        v = jnp.where(outside, 0.0, jnp.maximum(v, 0.0))
        if g == 0:
            v = jnp.where((lane < 32) & (s == 0), 0.0, v)
        if g == 4:
            v = jnp.where((lane >= 64) | ((lane >= 32) & (s == NSX - 1)), 0.0, v)
        eh_ref[g] = v.astype(BF)
    for cell in range(2):
        m = best[cell].astype(BF).astype(F32)
        for shift in (64, 32, 16, -1, -2, -4):
            m = jnp.maximum(m, roll(m, shift))
        best[cell] = m
    first = lane == 0
    both = [jnp.where(first, best[0], roll(best[1], 1)), jnp.where(first, roll(best[0], -8), roll(best[1], -7))]
    pool_ref[...] = jnp.transpose(jnp.concatenate(both, axis=0))[:8]


def k_decode(em_ref, eh_ref, w_ref, bias_ref, d_ref, xm, g_ref):
    lane = lanes_of(C)
    z = jnp.bitwise_and(lane, 15)
    for r in range(18):
        eh = eh_ref[r // 4]
        q = r % 4
        y_taps(em_ref[r], eh, 32 * q, eh, 32 * q + 16, xm, r, lane, z)
    products(w_ref, xm, g_ref, 0, 18)
    bias = bias_ref[...]
    for x in range(16):
        d_ref[x] = g_ref[x, pl.ds(0, C), :] + g_ref[x + 1, pl.ds(C, C), :] + g_ref[x + 2, pl.ds(2 * C, C), :] + bias


def k_message(inner_ref, own_ref, outer_ref, _d, _w, out_ref):
    even = even_of("sx")
    inner, outer = inner_ref[0:2], outer_ref[0:2]
    left, right = jnp.where(even, outer, inner), jnp.where(even, inner, outer)
    message = jnp.concatenate([left, own_ref[0:2], right, jnp.zeros((2, 128), F32)], axis=0)
    for i in range(NSY):
        out_ref[i] = message


def k_bottleneck(p_ref, vt_ref, bb_ref, ow_ref, out_ref):
    p = p_ref[...]
    pieces = []
    none = jnp.zeros((1, 8, 128), F32)
    for a in range(3):
        moved = p if a == 0 else jnp.concatenate([p[:, a:], p[:, :a]], axis=1)
        for b in range(3):
            if b == 0:
                v = jnp.concatenate([none, moved[:-1]], axis=0)
            elif b == 1:
                v = moved
            else:
                v = jnp.concatenate([moved[1:], none], axis=0)
            pieces.append(v.reshape(128, 128).astype(BF))
    h = dot_nt(jnp.concatenate(pieces, axis=1), vt_ref[...])
    h = jnp.maximum(h + bb_ref[...], 0.0).astype(BF)
    low = dot(h, ow_ref[...]).astype(BF).astype(F32)
    zero = jnp.zeros((8, 128), F32)
    for i in range(NSY):
        before = low[8 * (i - 1) : 8 * i] if i else zero
        after = low[8 * (i + 1) : 8 * (i + 2)] if i < NSY - 1 else zero
        out_ref[i] = jnp.concatenate([before, low[8 * i : 8 * i + 8], after], axis=0).astype(BF)


def k_final(parts_ref, s_ref, w_ref, d_ref, out_ref, xt, q_ref, buf):
    total = parts_ref[0].astype(F32)
    for i in range(1, NSY):
        total = total + parts_ref[i].astype(F32)
    total = jnp.concatenate([total, jnp.zeros((104, 128), F32)], axis=0)
    lt = jnp.transpose(total)
    lane = lanes_of(C)
    left = []
    for cell in range(4):
        here = jnp.bitwise_and(lane, 7) == cell
        left.append(jnp.concatenate([jnp.where(here, lt[:C], 0.0), jnp.where(here, lt[C:], 0.0)], axis=1).astype(BF))
    t = dot(jnp.concatenate(left, axis=0), s_ref[...])
    for cell in range(4):
        for bc in range(9):
            xt[cell, pl.ds(C * bc, C), :] = t[
                C * cell : C * cell + C, 128 * bc : 128 * bc + 128
            ].astype(BF)
    products(w_ref, xt, q_ref, 0, 4)
    s = lax.axis_index("sx")
    for x in range(16):
        v = d_ref[x]
        for a in range(3):
            g = x + a - 1
            num = 2 * g - 7
            low = num // 16
            high = (num - 16 * low) / 16.0
            cell = low + 1
            w_low, w_high = jnp.float32(1.0 - high), jnp.float32(high)
            first, last = s == 0, s == NSX - 1
            if cell == 0:
                w_low = jnp.where(first, 0.0, w_low)
                w_high = jnp.where(first, 0.0 if g < 0 else 1.0, w_high)
            if cell == 2:
                w_low = jnp.where(last, 0.0 if g > 15 else 1.0, w_low)
                w_high = jnp.where(last, 0.0, w_high)
            v = v + w_low * q_ref[cell, pl.ds(C * a, C), :]
            v = v + w_high * q_ref[cell + 1, pl.ds(C * a, C), :]
        buf[pl.ds(x, C, stride=16), :] = v
    out_ref[...] = buf[...].reshape(C, 16, 128).astype(BF)


def swapped(v, axis, start):
    size = lax.axis_size(axis)
    low = range(start, size - 1, 2)
    return lax.ppermute(v, axis, [(i, i + 1) for i in low] + [(i + 1, i) for i in low])


def per_device(features, enc_weight, enc_bias, proj_weight, bottle_weight, bottle_bias, out_weight, dec_weight, dec_bias):
    ft, inner, outer = call(
        k_features,
        (S((18, C, 128), BF), S((2, C, 128), BF), S((2, C, 128), BF)),
        features,
        name="features",
        scratch=[pltpu.VMEM((C * 16, 128), F32)],
    )
    outer, inner = swapped(outer, "sx", 1), swapped(inner, "sx", 0)
    we, be = call(
        k_enc_weights,
        (S((3 * C, 9 * C), BF), S((C, 128), F32)),
        enc_weight.reshape(27, C, C),
        enc_bias.reshape(1, C),
        name="enc_weights",
        flops=10**8,
    )
    xh, fl, fr, inner, outer = call(
        k_faces, (S((4, C, 128), BF),) + (S((5, C, 128), BF),) * 4, inner, outer, ft, name="faces"
    )
    outer, inner = swapped(outer, "sy", 1), swapped(inner, "sy", 0)
    wd, bd, vt, ow2, bb2, smat = call(
        k_dec_weights,
        (
            S((3 * C, 9 * C), BF),
            S((C, 128), F32),
            S((C, 9 * 128), BF),
            S((C, 128), BF),
            S((1, C), F32),
            S((256, 9 * 128), BF),
        ),
        dec_weight.reshape(27, C, C),
        dec_bias.reshape(1, C),
        bottle_weight.reshape(27 * 32, 512),
        proj_weight,
        out_weight,
        bottle_bias.reshape(1, 32),
        name="dec_weights",
        flops=4 * 10**8,
    )
    em, eh, pooled = call(
        k_encode,
        (S((18, C, 128), BF), S((5, C, 128), BF), S((8, 128), F32)),
        ft,
        xh,
        fl,
        fr,
        inner,
        outer,
        we,
        be,
        name="encode",
        scratch=[pltpu.VMEM((25, 9 * C, 128), BF), pltpu.VMEM((25, 3 * C, 128), F32)],
    )
    outer, inner = swapped(pooled, "sx", 1), swapped(pooled, "sx", 0)
    d = call(
        k_decode,
        S((16, C, 128), F32),
        em,
        eh,
        wd,
        bd,
        name="decode",
        scratch=[pltpu.VMEM((18, 9 * C, 128), BF), pltpu.VMEM((18, 3 * C, 128), F32)],
        flops=4 * 10**8,
    )
    message = call(k_message, S((NSY, 8, 128), F32), inner, pooled, outer, d, vt, name="message")
    everyone = lax.all_to_all(message, "sy", 0, 0, tiled=True)
    partial = call(k_bottleneck, S((NSY, 24, 128), BF), everyone, vt, bb2, ow2, name="bottleneck")
    parts = lax.all_to_all(partial, "sy", 0, 0, tiled=True)
    return call(
        k_final,
        S((C, 16, 128), BF),
        parts,
        smat,
        wd,
        d,
        name="final",
        scratch=[
            pltpu.VMEM((4, 9 * C, 128), BF),
            pltpu.VMEM((4, 3 * C, 128), F32),
            pltpu.VMEM((C * 16, 128), F32),
        ],
    )


def solution(mesh):
    in_specs = (P(None, "sx", "sy"), P(), P(), P(), P(None, None, None, "sy", None), P("sy"), P("sy", None), P(), P())
    return jax.shard_map(per_device, mesh=mesh, in_specs=in_specs, out_specs=P(None, "sx", "sy"), check_vma=False)
```

```python
import jax
import jax.numpy as jnp
from jax import lax
from jax.experimental import pallas as pl
from jax.experimental.pallas import tpu as pltpu
from jax.sharding import PartitionSpec as P


F32 = jnp.float32
BF = jnp.bfloat16
C = 64
NSX = 32
NSY = 16


def call(kernel, outs, *ins, scratch=(), flops=1000000, limit=16, in_space=pltpu.VMEM, out_space=pltpu.VMEM):
    return pl.pallas_call(
        kernel,
        out_shape=outs,
        in_specs=[pl.BlockSpec(memory_space=in_space)] * len(ins),
        out_specs=jax.tree.map(lambda _: pl.BlockSpec(memory_space=out_space), outs),
        scratch_shapes=list(scratch),
        compiler_params=pltpu.CompilerParams(vmem_limit_bytes=limit * 2**20),
        cost_estimate=pl.CostEstimate(flops=flops, transcendentals=0, bytes_accessed=100000),
    )(*ins)


def S(shape, dtype):
    return jax.ShapeDtypeStruct(shape, dtype)


def dot(a, b):
    return jnp.dot(a, b, preferred_element_type=F32)


def dot_nt(a, b):
    return lax.dot_general(a, b, (((1,), (1,)), ((), ())), preferred_element_type=F32)


def lanes_of(rows):
    return lax.broadcasted_iota(jnp.int32, (rows, 128), 1)


def roll(v, shift):
    shift = shift % 128
    return v if shift == 0 else pltpu.roll(v, shift, 1)


def even_of(axis):
    return lax.rem(lax.axis_index(axis), 2) == 0


def k_features(x_ref, ft_ref, inner_ref, outer_ref, buf):
    buf[...] = x_ref[...].reshape(C * 16, 128).astype(F32)
    even = even_of("sx")

    def row(x):
        return buf[pl.ds(x, C, stride=16), :]

    for k in range(2):
        low, high = row(k), row(14 + k)
        inner_ref[k] = jnp.where(even, high, low).astype(BF)
        outer_ref[k] = jnp.where(even, low, high).astype(BF)
    for x in range(16):
        ft_ref[x + 2] = row(x).astype(BF)


def k_faces(inner_ref, outer_ref, ft_ref, x_ref, left_ref, right_ref, s_inner_ref, s_outer_ref):
    lane = lanes_of(C)
    even_x, even_y = even_of("sx"), even_of("sy")
    for k in range(2):
        inner, outer = inner_ref[k], outer_ref[k]
        x_ref[k] = jnp.where(even_x, outer, inner)
        x_ref[2 + k] = jnp.where(even_x, inner, outer)
    for g in range(5):
        left = None
        for q in range(4):
            r = 4 * g + q
            v = x_ref[r] if r < 2 else ft_ref[r] if r < 18 else x_ref[r - 16]
            v = v.astype(F32)
            a, b = roll(v, 32 * q), roll(v, 32 * q - 96)
            if q == 0:
                left, right = a, b
            else:
                here = lane >= 32 * q
                left, right = jnp.where(here, a, left), jnp.where(here, b, right)
        left_ref[g] = left.astype(BF)
        right_ref[g] = right.astype(BF)
        s_inner_ref[g] = jnp.where(even_y, right, left).astype(BF)
        s_outer_ref[g] = jnp.where(even_y, left, right).astype(BF)


def arranged(w_ref, out_ref, taps):
    for a in range(3):
        for at in range(0, len(taps), 2):
            blocks = [w_ref[a * 9 + t] for t in taps[at : at + 2]]
            wide = blocks[0] if len(blocks) == 1 else jnp.concatenate(blocks, axis=1)
            out_ref[pl.ds(a * C, C), pl.ds(C * at, wide.shape[1])] = wide


def column(b_ref):
    row = jnp.broadcast_to(b_ref[...], (C, C))
    same = lax.broadcasted_iota(jnp.int32, (C, C), 0) == lax.broadcasted_iota(jnp.int32, (C, C), 1)
    return jnp.broadcast_to(jnp.sum(jnp.where(same, row, 0.0), axis=1, keepdims=True), (C, 128))


def interp_weight(g, cell, count, cells):
    num = 2 * g - 7
    low = jnp.right_shift(num, 4)
    w = (num - 16 * low).astype(F32) * (1.0 / 16.0)
    w = jnp.where((low < 0) | (low >= cells - 1), 0.0, w)
    low = jnp.clip(low, 0, cells - 1)
    value = jnp.where(cell == low, 1.0 - w, jnp.where(cell == low + 1, w, 0.0))
    return jnp.where((g >= 0) & (g < count), value, 0.0)


def k_weights(*refs):
    hbm, outs, held, sem = refs[:8], refs[8:17], refs[17:25], refs[25]
    copies = [pltpu.make_async_copy(h, v, sem.at[i]) for i, (h, v) in enumerate(zip(hbm, held))]
    for c in copies:
        c.start()
    ew, eb, dw, db, bw, proj, ow, bb = held
    we_ref, wedge_ref, be_ref, wd_ref, bd_ref, vt_ref, ow2_ref, bb2_ref, s_ref = outs
    j = lax.axis_index("sy")
    row = lax.broadcasted_iota(jnp.int32, (32, 128), 0)
    lane = lax.broadcasted_iota(jnp.int32, (32, 128), 1)
    y, z = jnp.right_shift(lane, 4), jnp.bitwise_and(lane, 15)
    cell_y = j - 1 + jnp.right_shift(row, 3)
    zero = jnp.zeros((96, 128), BF)
    for b in range(3):
        wy = interp_weight(8 * j + y + (b - 1), cell_y, 8 * NSY, NSY)
        wy = jnp.where(row < 24, wy, 0.0)
        for c in range(3):
            for zo in range(2):
                wz = interp_weight(z + (c - 1), 1 - zo, 16, 2)
                at = pl.ds(128 * (3 * b + c), 128)
                s_ref[pl.ds(128 * zo, 32), at] = (wy * wz).astype(BF)
                s_ref[pl.ds(128 * zo + 32, 96), at] = zero
    for c in copies:
        c.wait()
    arranged(ew, we_ref, range(9))
    arranged(ew, wedge_ref, (0, 1, 2, 6, 7, 8))
    arranged(dw, wd_ref, range(9))
    be_ref[...] = column(eb)
    bd_ref[...] = column(db)
    p = proj[...]
    r = dot_nt(bw[...], jnp.concatenate([p, p], axis=0))
    half = lanes_of(C) < C
    for ab in range(9):
        both = jnp.where(half, r[96 * ab : 96 * ab + 64], r[96 * ab + 32 : 96 * ab + 96])
        vt_ref[:, pl.ds(128 * ab, 128)] = both.astype(BF)
    o = ow[...]
    none = jnp.zeros_like(o)
    ow2_ref[...] = jnp.concatenate([jnp.concatenate([o, none], axis=1), jnp.concatenate([none, o], axis=1)], axis=0)
    bb2_ref[...] = jnp.concatenate([bb[...], bb[...]], axis=1)


def taps_of(v, z):
    zero = jnp.zeros_like(v)
    return [jnp.where(z == 0, zero, roll(v, 1)), v, jnp.where(z == 15, zero, roll(v, -1))]


def put_taps(parts, xm, n, z):
    for b, v in enumerate(parts):
        for c, tap in enumerate(taps_of(v, z)):
            xm[n, 3 * b + c, pl.ds(0, C), :] = tap


def products(w_ref, xm, first, last, store):
    w = w_ref[...]

    def block(n):
        return jnp.concatenate([xm[n, t, pl.ds(0, C), :] for t in range(9)], axis=0)

    for n in range(first, last, 2):
        if n + 1 < last:
            g = dot(w, jnp.concatenate([block(n), block(n + 1)], axis=1))
            store(n, g[:, :128])
            store(n + 1, g[:, 128:])
        else:
            store(n, dot(w, block(n)))


def into(g_ref):
    def store(n, g):
        g_ref[n, pl.ds(0, 3 * C), :] = g

    return store


def summed(g_ref, r):
    return g_ref[r, pl.ds(0, C), :] + g_ref[r + 1, pl.ds(C, C), :] + g_ref[r + 2, pl.ds(2 * C, C), :]


def summed_packed(packed, g, lane):
    v = packed[g][:C]
    for a in (1, 2):
        this, after = packed[g][a * C : a * C + C], packed[min(g + 1, 4)][a * C : a * C + C]
        v = v + roll(jnp.where(lane < 32 * a, after, this), -32 * a)
    return v


def packed_products(w, blocks):
    out = []
    for n in range(0, 5, 2):
        if n + 1 < 5:
            g = dot(w, jnp.concatenate([blocks[n], blocks[n + 1]], axis=1))
            out += [g[:, :128], g[:, 128:]]
        else:
            out.append(dot(w, blocks[n]))
    return out


def y_halos(inner_ref, outer_ref, g):
    even_y = even_of("sy")
    inner, outer = inner_ref[g], outer_ref[g]
    return jnp.where(even_y, outer, inner), jnp.where(even_y, inner, outer)


def k_interior(ft_ref, x_ref, w_ref, g_ref, xm):
    lane = lanes_of(C)
    z = jnp.bitwise_and(lane, 15)
    for r in range(20):
        v = x_ref[r] if r < 2 else ft_ref[r] if r < 18 else x_ref[r - 16]
        zero = jnp.zeros_like(v)
        put_taps(
            [jnp.where(lane < 16, zero, roll(v, 16)), v, jnp.where(lane >= 112, zero, roll(v, -16))], xm, r, z
        )
    products(w_ref, xm, 0, 20, into(g_ref))


def k_encode(g_ref, inner_ref, outer_ref, w_ref, bias_ref, em_ref, pool_ref):
    lane = lanes_of(C)
    z = jnp.bitwise_and(lane, 15)
    even = jnp.bitwise_and(lane, 16) == 0
    edge = (lane < 16) | (lane >= 112)
    s = lax.axis_index("sx")
    blocks = []
    for g in range(5):
        hl, hr = y_halos(inner_ref, outer_ref, g)
        zero = jnp.zeros_like(hl)
        low, high = jnp.where(even, zero, hl), jnp.where(even, hr, zero)
        blocks.append(jnp.concatenate(taps_of(low, z) + taps_of(high, z), axis=0))
    packed = packed_products(w_ref[...], blocks)
    bias = bias_ref[...]
    best = [None, None]
    for r in range(18):
        if r % 4 == 0:
            at_edge = summed_packed(packed, r // 4, lane)
        v = summed(g_ref, r) + bias
        v = v + jnp.where(edge, roll(at_edge, -(32 * (r % 4) + 16)), 0.0)
        v = jnp.maximum(v, 0.0)
        if r == 0:
            v = jnp.where(s == 0, 0.0, v)
        if r == 17:
            v = jnp.where(s == NSX - 1, 0.0, v)
        em_ref[r] = v.astype(BF)
        if 1 <= r <= 16:
            cell = (r - 1) // 8
            best[cell] = v if best[cell] is None else jnp.maximum(best[cell], v)
    for cell in range(2):
        m = best[cell].astype(BF).astype(F32)
        for shift in (64, 32, 16, -1, -2, -4):
            m = jnp.maximum(m, roll(m, shift))
        best[cell] = m
    first = lane == 0
    both = [jnp.where(first, best[0], roll(best[1], 1)), jnp.where(first, roll(best[0], -8), roll(best[1], -7))]
    pool_ref[...] = jnp.transpose(jnp.concatenate(both, axis=0))[:8]


def k_decode(
    fl_ref, fr_ref, inner_ref, outer_ref, em_ref, we_ref, be_ref, w_ref, bias_ref, d_ref, xm, g_ref
):
    lane = lanes_of(C)
    z = jnp.bitwise_and(lane, 15)
    even = jnp.bitwise_and(lane, 16) == 0
    s, j = lax.axis_index("sx"), lax.axis_index("sy")
    blocks = []
    for g in range(5):
        hl, hr = y_halos(inner_ref, outer_ref, g)
        fl, fr = fl_ref[g], fr_ref[g]
        parts = [
            jnp.where(even, roll(fr, -16), roll(hl, 16)),
            jnp.where(even, hr, hl),
            jnp.where(even, roll(hr, -16), roll(fl, 16)),
        ]
        blocks.append(jnp.concatenate([tap for v in parts for tap in taps_of(v, z)], axis=0))
    packed = packed_products(we_ref[...], blocks)
    outside = (even & (j == NSY - 1)) | (~even & (j == 0))
    halo = []
    for g in range(5):
        v = summed_packed(packed, g, lane) + be_ref[...]
        v = jnp.where(outside, 0.0, jnp.maximum(v, 0.0))
        if g == 0:
            v = jnp.where((lane < 32) & (s == 0), 0.0, v)
        if g == 4:
            v = jnp.where((lane >= 64) | ((lane >= 32) & (s == NSX - 1)), 0.0, v)
        halo.append(v.astype(BF))
    for r in range(18):
        v = em_ref[r]
        beside = roll(halo[r // 4], -(32 * (r % 4) + 16))
        put_taps(
            [jnp.where(lane < 16, beside, roll(v, 16)), v, jnp.where(lane >= 112, beside, roll(v, -16))], xm, r, z
        )
    products(w_ref, xm, 0, 18, into(g_ref))
    bias = bias_ref[...]
    for x in range(16):
        d_ref[x] = summed(g_ref, x) + bias


def k_message(inner_ref, own_ref, outer_ref, _d, out_ref):
    even = even_of("sx")
    inner, outer = inner_ref[0:2], outer_ref[0:2]
    left, right = jnp.where(even, outer, inner), jnp.where(even, inner, outer)
    message = jnp.concatenate([left, own_ref[0:2], right, jnp.zeros((2, 128), F32)], axis=0)
    for i in range(NSY):
        out_ref[i] = message


def k_bottleneck(p_ref, vt_ref, bb_ref, ow_ref, out_ref):
    p = p_ref[...]
    pieces = []
    none = jnp.zeros((1, 8, 128), F32)
    for a in range(3):
        moved = p if a == 0 else jnp.concatenate([p[:, a:], p[:, :a]], axis=1)
        for b in range(3):
            if b == 0:
                v = jnp.concatenate([none, moved[:-1]], axis=0)
            elif b == 1:
                v = moved
            else:
                v = jnp.concatenate([moved[1:], none], axis=0)
            pieces.append(v.reshape(128, 128).astype(BF))
    h = dot_nt(jnp.concatenate(pieces, axis=1), vt_ref[...])
    h = jnp.maximum(h + bb_ref[...], 0.0).astype(BF)
    low = dot(h, ow_ref[...]).astype(BF).astype(F32)
    zero = jnp.zeros((8, 128), F32)
    for i in range(NSY):
        before = low[8 * (i - 1) : 8 * i] if i else zero
        after = low[8 * (i + 1) : 8 * (i + 2)] if i < NSY - 1 else zero
        out_ref[i] = jnp.concatenate([before, low[8 * i : 8 * i + 8], after], axis=0).astype(BF)


def k_final(parts_ref, s_ref, w_ref, d_ref, out_ref, xt, q_ref, buf, done, sem):
    total = parts_ref[0].astype(F32)
    for i in range(1, NSY):
        total = total + parts_ref[i].astype(F32)
    total = jnp.concatenate([total, jnp.zeros((104, 128), F32)], axis=0)
    lt = jnp.transpose(total)
    lane = lanes_of(C)
    left = []
    for cell in range(4):
        here = jnp.bitwise_and(lane, 7) == cell
        left.append(jnp.concatenate([jnp.where(here, lt[:C], 0.0), jnp.where(here, lt[C:], 0.0)], axis=1).astype(BF))
    t = dot(jnp.concatenate(left, axis=0), s_ref[...])
    for cell in range(4):
        for bc in range(9):
            xt[cell, bc, pl.ds(0, C), :] = t[C * cell : C * cell + C, 128 * bc : 128 * bc + 128].astype(BF)
    products(w_ref, xt, 0, 4, into(q_ref))
    s = lax.axis_index("sx")
    first, last = s == 0, s == NSX - 1
    copies = []
    for part in range(4):
        rows = 16
        for x in range(16):
            v = d_ref[x, pl.ds(rows * part, rows), :]
            for a in range(3):
                g = x + a - 1
                num = 2 * g - 7
                low = num // 16
                high = (num - 16 * low) / 16.0
                cell = low + 1
                w_low, w_high = jnp.float32(1.0 - high), jnp.float32(high)
                if cell == 0:
                    w_low = jnp.where(first, 0.0, w_low)
                    w_high = jnp.where(first, 0.0 if g < 0 else 1.0, w_high)
                if cell == 2:
                    w_low = jnp.where(last, 0.0 if g > 15 else 1.0, w_low)
                    w_high = jnp.where(last, 0.0, w_high)
                at = pl.ds(C * a + rows * part, rows)
                v = v + w_low * q_ref[cell, at, :]
                v = v + w_high * q_ref[cell + 1, at, :]
            buf[part, pl.ds(x, rows, stride=16), :] = v
        at = pl.ds(rows * part, rows)
        done[at] = buf[part].reshape(rows, 16, 128).astype(BF)
        copy = pltpu.make_async_copy(done.at[at], out_ref.at[at], sem.at[part])
        copy.start()
        copies.append(copy)
    for copy in copies:
        copy.wait()


def swapped(v, axis, start):
    size = lax.axis_size(axis)
    low = range(start, size - 1, 2)
    return lax.ppermute(v, axis, [(i, i + 1) for i in low] + [(i + 1, i) for i in low])


def per_device(features, enc_weight, enc_bias, proj_weight, bottle_weight, bottle_bias, out_weight, dec_weight, dec_bias):
    ft, inner, outer = call(
        k_features,
        (S((18, C, 128), BF), S((2, C, 128), BF), S((2, C, 128), BF)),
        features,
        scratch=[pltpu.VMEM((C * 16, 128), F32)],
    )
    outer, inner = swapped(outer, "sx", 1), swapped(inner, "sx", 0)
    sources = (
        enc_weight.reshape(27, C, C),
        enc_bias.reshape(1, C),
        dec_weight.reshape(27, C, C),
        dec_bias.reshape(1, C),
        bottle_weight.reshape(27 * 32, 512),
        proj_weight,
        out_weight,
        bottle_bias.reshape(1, 32),
    )
    sources = tuple(pltpu.with_memory_space_constraint(v, pltpu.HBM) for v in sources)
    we, wedge, be, wd, bd, vt, ow2, bb2, smat = call(
        k_weights,
        (
            S((3 * C, 9 * C), BF),
            S((3 * C, 6 * C), BF),
            S((C, 128), F32),
            S((3 * C, 9 * C), BF),
            S((C, 128), F32),
            S((C, 9 * 128), BF),
            S((C, 128), BF),
            S((1, C), F32),
            S((256, 9 * 128), BF),
        ),
        *sources,
        scratch=[pltpu.VMEM(v.shape, v.dtype) for v in sources] + [pltpu.SemaphoreType.DMA((8,))],
        flops=4 * 10**8,
        in_space=pltpu.HBM,
    )
    xh, fl, fr, inner, outer = call(k_faces, (S((4, C, 128), BF),) + (S((5, C, 128), BF),) * 4, inner, outer, ft)
    outer, inner = swapped(outer, "sy", 1), swapped(inner, "sy", 0)
    product = call(
        k_interior,
        S((20, 3 * C + 8, 128), F32),
        ft,
        xh,
        we,
        scratch=[pltpu.VMEM((20, 9, C + 16, 128), BF)],
        flops=4 * 10**8,
    )
    em, pooled = call(k_encode, (S((18, C, 128), BF), S((8, 128), F32)), product, inner, outer, wedge, be)
    p_outer, p_inner = swapped(pooled, "sx", 1), swapped(pooled, "sx", 0)
    d = call(
        k_decode,
        S((16, C, 128), F32),
        fl,
        fr,
        inner,
        outer,
        em,
        we,
        be,
        wd,
        bd,
        scratch=[pltpu.VMEM((18, 9, C + 16, 128), BF), pltpu.VMEM((18, 3 * C + 8, 128), F32)],
        flops=4 * 10**8,
    )
    message = call(k_message, S((NSY, 8, 128), F32), p_inner, pooled, p_outer, d)
    everyone = lax.all_to_all(message, "sy", 0, 0, tiled=True)
    partial = call(k_bottleneck, S((NSY, 24, 128), BF), everyone, vt, bb2, ow2)
    parts = lax.all_to_all(partial, "sy", 0, 0, tiled=True)
    return call(
        k_final,
        S((C, 16, 128), BF),
        parts,
        smat,
        wd,
        d,
        scratch=[
            pltpu.VMEM((4, 9, C + 16, 128), BF),
            pltpu.VMEM((4, 3 * C + 8, 128), F32),
            pltpu.VMEM((4, 256, 128), F32),
            pltpu.VMEM((C, 16, 128), BF),
            pltpu.SemaphoreType.DMA((4,)),
        ],
        out_space=pltpu.HBM,
    )


def solution(mesh):
    in_specs = (P(None, "sx", "sy"), P(), P(), P(), P(None, None, None, "sy", None), P("sy"), P("sy", None), P(), P())

    return jax.shard_map(per_device, mesh=mesh, in_specs=in_specs, out_specs=P(None, "sx", "sy"), check_vma=False)
```

```python
import jax
import jax.numpy as jnp
from jax import lax
from jax.experimental import pallas as pl
from jax.experimental.pallas import tpu as pltpu
from jax.sharding import PartitionSpec as P


F32 = jnp.float32
BF = jnp.bfloat16
C = 64
NSX = 32
NSY = 16


def call(kernel, outs, *ins, scratch=(), flops=1000000, limit=16, hbm=(), out_space=pltpu.VMEM):
    ins = [pltpu.with_memory_space_constraint(v, pltpu.HBM) if i in hbm else v for i, v in enumerate(ins)]
    return pl.pallas_call(
        kernel,
        out_shape=outs,
        in_specs=[pl.BlockSpec(memory_space=pltpu.HBM if i in hbm else pltpu.VMEM) for i in range(len(ins))],
        out_specs=jax.tree.map(lambda _: pl.BlockSpec(memory_space=out_space), outs),
        scratch_shapes=list(scratch),
        compiler_params=pltpu.CompilerParams(vmem_limit_bytes=limit * 2**20),
        cost_estimate=pl.CostEstimate(flops=flops, transcendentals=0, bytes_accessed=100000),
    )(*ins)


def S(shape, dtype):
    return jax.ShapeDtypeStruct(shape, dtype)


def dot(a, b):
    return jnp.dot(a, b, preferred_element_type=F32)


def dot_nt(a, b):
    return lax.dot_general(a, b, (((1,), (1,)), ((), ())), preferred_element_type=F32)


def lanes_of(rows):
    return lax.broadcasted_iota(jnp.int32, (rows, 128), 1)


def roll(v, shift):
    shift = shift % 128
    return v if shift == 0 else pltpu.roll(v, shift, 1)


def even_of(axis):
    return lax.rem(lax.axis_index(axis), 2) == 0


def fetches(sources, targets, sem):
    copies = [pltpu.make_async_copy(a, b, sem.at[i]) for i, (a, b) in enumerate(zip(sources, targets))]
    for copy in copies:
        copy.start()
    return copies


def k_features(x_ref, ew_hbm, eb_hbm, ft_ref, inner_ref, outer_ref, ew_ref, eb_ref, held, buf, sem):
    copies = fetches((x_ref, ew_hbm, eb_hbm), (held, ew_ref, eb_ref), sem)
    even = even_of("sx")
    copies[0].wait()
    buf[...] = held[...].reshape(C * 16, 128).astype(F32)

    def row(x):
        return buf[pl.ds(x, C, stride=16), :]

    for k in range(2):
        low, high = row(k), row(14 + k)
        inner_ref[k] = jnp.where(even, high, low).astype(BF)
        outer_ref[k] = jnp.where(even, low, high).astype(BF)
    for x in range(16):
        ft_ref[x + 2] = row(x).astype(BF)
    for copy in copies[1:]:
        copy.wait()


def k_faces(inner_ref, outer_ref, ft_ref, x_ref, left_ref, right_ref, s_inner_ref, s_outer_ref):
    lane = lanes_of(C)
    even_x, even_y = even_of("sx"), even_of("sy")
    for k in range(2):
        inner, outer = inner_ref[k], outer_ref[k]
        x_ref[k] = jnp.where(even_x, outer, inner)
        x_ref[2 + k] = jnp.where(even_x, inner, outer)
    for g in range(5):
        left = None
        for q in range(4):
            r = 4 * g + q
            v = x_ref[r] if r < 2 else ft_ref[r] if r < 18 else x_ref[r - 16]
            v = v.astype(F32)
            a, b = roll(v, 32 * q), roll(v, 32 * q - 96)
            if q == 0:
                left, right = a, b
            else:
                here = lane >= 32 * q
                left, right = jnp.where(here, a, left), jnp.where(here, b, right)
        left_ref[g] = left.astype(BF)
        right_ref[g] = right.astype(BF)
        s_inner_ref[g] = jnp.where(even_y, right, left).astype(BF)
        s_outer_ref[g] = jnp.where(even_y, left, right).astype(BF)


def arranged(w_ref, out_ref, taps):
    for a in range(3):
        for at in range(0, len(taps), 2):
            blocks = [w_ref[a * 9 + t] for t in taps[at : at + 2]]
            wide = blocks[0] if len(blocks) == 1 else jnp.concatenate(blocks, axis=1)
            out_ref[pl.ds(a * C, C), pl.ds(C * at, wide.shape[1])] = wide


def column(b_ref):
    row = jnp.broadcast_to(b_ref[...], (C, C))
    same = lax.broadcasted_iota(jnp.int32, (C, C), 0) == lax.broadcasted_iota(jnp.int32, (C, C), 1)
    return jnp.broadcast_to(jnp.sum(jnp.where(same, row, 0.0), axis=1, keepdims=True), (C, 128))


def interp_weight(g, cell, count, cells):
    num = 2 * g - 7
    low = jnp.right_shift(num, 4)
    w = (num - 16 * low).astype(F32) * (1.0 / 16.0)
    w = jnp.where((low < 0) | (low >= cells - 1), 0.0, w)
    low = jnp.clip(low, 0, cells - 1)
    value = jnp.where(cell == low, 1.0 - w, jnp.where(cell == low + 1, w, 0.0))
    return jnp.where((g >= 0) & (g < count), value, 0.0)


def k_enc_weights(ew, eb, we_ref, wedge_ref, be_ref):
    arranged(ew, we_ref, range(9))
    arranged(ew, wedge_ref, (0, 1, 2, 6, 7, 8))
    be_ref[...] = column(eb)


def k_weights(dw, db, bw, proj, ow, bb, wd_ref, bd_ref, vt_ref, ow2_ref, bb2_ref, s_ref):
    j = lax.axis_index("sy")
    row = lax.broadcasted_iota(jnp.int32, (32, 128), 0)
    lane = lax.broadcasted_iota(jnp.int32, (32, 128), 1)
    y, z = jnp.right_shift(lane, 4), jnp.bitwise_and(lane, 15)
    cell_y = j - 1 + jnp.right_shift(row, 3)
    zero = jnp.zeros((96, 128), BF)
    for b in range(3):
        wy = interp_weight(8 * j + y + (b - 1), cell_y, 8 * NSY, NSY)
        wy = jnp.where(row < 24, wy, 0.0)
        for c in range(3):
            for zo in range(2):
                wz = interp_weight(z + (c - 1), 1 - zo, 16, 2)
                at = pl.ds(128 * (3 * b + c), 128)
                s_ref[pl.ds(128 * zo, 32), at] = (wy * wz).astype(BF)
                s_ref[pl.ds(128 * zo + 32, 96), at] = zero
    arranged(dw, wd_ref, range(9))
    bd_ref[...] = column(db)
    p = proj[...]
    r = dot_nt(bw[...], jnp.concatenate([p, p], axis=0))
    half = lanes_of(C) < C
    for ab in range(9):
        both = jnp.where(half, r[96 * ab : 96 * ab + 64], r[96 * ab + 32 : 96 * ab + 96])
        vt_ref[:, pl.ds(128 * ab, 128)] = both.astype(BF)
    o = ow[...]
    none = jnp.zeros_like(o)
    ow2_ref[...] = jnp.concatenate([jnp.concatenate([o, none], axis=1), jnp.concatenate([none, o], axis=1)], axis=0)
    bb2_ref[...] = jnp.concatenate([bb[...], bb[...]], axis=1)


def taps_of(v, z):
    zero = jnp.zeros_like(v)
    return [jnp.where(z == 0, zero, roll(v, 1)), v, jnp.where(z == 15, zero, roll(v, -1))]


def put_taps(parts, xm, n, z):
    for b, v in enumerate(parts):
        for c, tap in enumerate(taps_of(v, z)):
            xm[n, 3 * b + c, pl.ds(0, C), :] = tap


def products(w_ref, xm, first, last, store):
    w = w_ref[...]

    def block(n):
        return jnp.concatenate([xm[n, t, pl.ds(0, C), :] for t in range(9)], axis=0)

    for n in range(first, last, 2):
        if n + 1 < last:
            g = dot(w, jnp.concatenate([block(n), block(n + 1)], axis=1))
            store(n, g[:, :128])
            store(n + 1, g[:, 128:])
        else:
            store(n, dot(w, block(n)))


def into(g_ref):
    def store(n, g):
        g_ref[n, pl.ds(0, 3 * C), :] = g

    return store


def summed(g_ref, r):
    return g_ref[r, pl.ds(0, C), :] + g_ref[r + 1, pl.ds(C, C), :] + g_ref[r + 2, pl.ds(2 * C, C), :]


def summed_packed(packed, g, lane):
    v = packed[g][:C]
    for a in (1, 2):
        this, after = packed[g][a * C : a * C + C], packed[min(g + 1, 4)][a * C : a * C + C]
        v = v + roll(jnp.where(lane < 32 * a, after, this), -32 * a)
    return v


def packed_products(w, blocks):
    out = []
    for n in range(0, 5, 2):
        if n + 1 < 5:
            g = dot(w, jnp.concatenate([blocks[n], blocks[n + 1]], axis=1))
            out += [g[:, :128], g[:, 128:]]
        else:
            out.append(dot(w, blocks[n]))
    return out


def y_halos(inner_ref, outer_ref, g):
    even_y = even_of("sy")
    inner, outer = inner_ref[g], outer_ref[g]
    return jnp.where(even_y, outer, inner), jnp.where(even_y, inner, outer)


def k_interior(ft_ref, x_ref, w_ref, *refs):
    sources, g_ref, targets, xm, sem = refs[:6], refs[6], refs[7:13], refs[13], refs[14]
    copies = fetches(sources, targets, sem)
    lane = lanes_of(C)
    z = jnp.bitwise_and(lane, 15)
    for r in range(20):
        v = x_ref[r] if r < 2 else ft_ref[r] if r < 18 else x_ref[r - 16]
        zero = jnp.zeros_like(v)
        put_taps(
            [jnp.where(lane < 16, zero, roll(v, 16)), v, jnp.where(lane >= 112, zero, roll(v, -16))], xm, r, z
        )
    products(w_ref, xm, 0, 20, into(g_ref))
    for copy in copies:
        copy.wait()


def k_encode(g_ref, inner_ref, outer_ref, w_ref, bias_ref, em_ref, pool_ref):
    lane = lanes_of(C)
    z = jnp.bitwise_and(lane, 15)
    even = jnp.bitwise_and(lane, 16) == 0
    edge = (lane < 16) | (lane >= 112)
    s = lax.axis_index("sx")
    blocks = []
    for g in range(5):
        hl, hr = y_halos(inner_ref, outer_ref, g)
        zero = jnp.zeros_like(hl)
        low, high = jnp.where(even, zero, hl), jnp.where(even, hr, zero)
        blocks.append(jnp.concatenate(taps_of(low, z) + taps_of(high, z), axis=0))
    packed = packed_products(w_ref[...], blocks)
    bias = bias_ref[...]
    best = [None, None]
    for r in range(18):
        if r % 4 == 0:
            at_edge = summed_packed(packed, r // 4, lane)
        v = summed(g_ref, r) + bias
        v = v + jnp.where(edge, roll(at_edge, -(32 * (r % 4) + 16)), 0.0)
        v = jnp.maximum(v, 0.0)
        if r == 0:
            v = jnp.where(s == 0, 0.0, v)
        if r == 17:
            v = jnp.where(s == NSX - 1, 0.0, v)
        em_ref[r] = v.astype(BF)
        if 1 <= r <= 16:
            cell = (r - 1) // 8
            best[cell] = v if best[cell] is None else jnp.maximum(best[cell], v)
    for cell in range(2):
        m = best[cell].astype(BF).astype(F32)
        for shift in (64, 32, 16, -1, -2, -4):
            m = jnp.maximum(m, roll(m, shift))
        best[cell] = m
    first = lane == 0
    both = [jnp.where(first, best[0], roll(best[1], 1)), jnp.where(first, roll(best[0], -8), roll(best[1], -7))]
    pool_ref[...] = jnp.transpose(jnp.concatenate(both, axis=0))[:8]


def k_decode(
    fl_ref, fr_ref, inner_ref, outer_ref, em_ref, we_ref, be_ref, w_ref, bias_ref, d_ref, xm, g_ref
):
    lane = lanes_of(C)
    z = jnp.bitwise_and(lane, 15)
    even = jnp.bitwise_and(lane, 16) == 0
    s, j = lax.axis_index("sx"), lax.axis_index("sy")
    blocks = []
    for g in range(5):
        hl, hr = y_halos(inner_ref, outer_ref, g)
        fl, fr = fl_ref[g], fr_ref[g]
        parts = [
            jnp.where(even, roll(fr, -16), roll(hl, 16)),
            jnp.where(even, hr, hl),
            jnp.where(even, roll(hr, -16), roll(fl, 16)),
        ]
        blocks.append(jnp.concatenate([tap for v in parts for tap in taps_of(v, z)], axis=0))
    packed = packed_products(we_ref[...], blocks)
    outside = (even & (j == NSY - 1)) | (~even & (j == 0))
    halo = []
    for g in range(5):
        v = summed_packed(packed, g, lane) + be_ref[...]
        v = jnp.where(outside, 0.0, jnp.maximum(v, 0.0))
        if g == 0:
            v = jnp.where((lane < 32) & (s == 0), 0.0, v)
        if g == 4:
            v = jnp.where((lane >= 64) | ((lane >= 32) & (s == NSX - 1)), 0.0, v)
        halo.append(v.astype(BF))
    for r in range(18):
        v = em_ref[r]
        beside = roll(halo[r // 4], -(32 * (r % 4) + 16))
        put_taps(
            [jnp.where(lane < 16, beside, roll(v, 16)), v, jnp.where(lane >= 112, beside, roll(v, -16))], xm, r, z
        )
    products(w_ref, xm, 0, 18, into(g_ref))
    bias = bias_ref[...]
    for x in range(16):
        d_ref[x] = summed(g_ref, x) + bias


def k_message(inner_ref, own_ref, outer_ref, _vt, out_ref):
    even = even_of("sx")
    inner, outer = inner_ref[0:2], outer_ref[0:2]
    left, right = jnp.where(even, outer, inner), jnp.where(even, inner, outer)
    message = jnp.concatenate([left, own_ref[0:2], right, jnp.zeros((2, 128), F32)], axis=0)
    for i in range(NSY):
        out_ref[i] = message


def k_bottleneck(p_ref, vt_ref, bb_ref, ow_ref, out_ref):
    p = p_ref[...]
    pieces = []
    none = jnp.zeros((1, 8, 128), F32)
    for a in range(3):
        moved = p if a == 0 else jnp.concatenate([p[:, a:], p[:, :a]], axis=1)
        for b in range(3):
            if b == 0:
                v = jnp.concatenate([none, moved[:-1]], axis=0)
            elif b == 1:
                v = moved
            else:
                v = jnp.concatenate([moved[1:], none], axis=0)
            pieces.append(v.reshape(128, 128).astype(BF))
    h = dot_nt(jnp.concatenate(pieces, axis=1), vt_ref[...])
    h = jnp.maximum(h + bb_ref[...], 0.0).astype(BF)
    low = dot(h, ow_ref[...]).astype(BF).astype(F32)
    zero = jnp.zeros((8, 128), F32)
    for i in range(NSY):
        before = low[8 * (i - 1) : 8 * i] if i else zero
        after = low[8 * (i + 1) : 8 * (i + 2)] if i < NSY - 1 else zero
        out_ref[i] = jnp.concatenate([before, low[8 * i : 8 * i + 8], after], axis=0).astype(BF)


def k_final(parts_ref, s_ref, w_ref, d_ref, out_ref, xt, q_ref, buf, done, sem):
    total = parts_ref[0].astype(F32)
    for i in range(1, NSY):
        total = total + parts_ref[i].astype(F32)
    total = jnp.concatenate([total, jnp.zeros((104, 128), F32)], axis=0)
    lt = jnp.transpose(total)
    lane = lanes_of(C)
    left = []
    for cell in range(4):
        here = jnp.bitwise_and(lane, 7) == cell
        left.append(jnp.concatenate([jnp.where(here, lt[:C], 0.0), jnp.where(here, lt[C:], 0.0)], axis=1).astype(BF))
    t = dot(jnp.concatenate(left, axis=0), s_ref[...])
    for cell in range(4):
        for bc in range(9):
            xt[cell, bc, pl.ds(0, C), :] = t[C * cell : C * cell + C, 128 * bc : 128 * bc + 128].astype(BF)
    products(w_ref, xt, 0, 4, into(q_ref))
    s = lax.axis_index("sx")
    first, last = s == 0, s == NSX - 1
    copies = []
    for part in range(4):
        rows = 16
        for x in range(16):
            v = d_ref[x, pl.ds(rows * part, rows), :]
            for a in range(3):
                g = x + a - 1
                num = 2 * g - 7
                low = num // 16
                high = (num - 16 * low) / 16.0
                cell = low + 1
                w_low, w_high = jnp.float32(1.0 - high), jnp.float32(high)
                if cell == 0:
                    w_low = jnp.where(first, 0.0, w_low)
                    w_high = jnp.where(first, 0.0 if g < 0 else 1.0, w_high)
                if cell == 2:
                    w_low = jnp.where(last, 0.0 if g > 15 else 1.0, w_low)
                    w_high = jnp.where(last, 0.0, w_high)
                at = pl.ds(C * a + rows * part, rows)
                v = v + w_low * q_ref[cell, at, :]
                v = v + w_high * q_ref[cell + 1, at, :]
            buf[part, pl.ds(x, rows, stride=16), :] = v
        at = pl.ds(rows * part, rows)
        done[at] = buf[part].reshape(rows, 16, 128).astype(BF)
        copy = pltpu.make_async_copy(done.at[at], out_ref.at[at], sem.at[part])
        copy.start()
        copies.append(copy)
    for copy in copies:
        copy.wait()


def swapped(v, axis, start):
    size = lax.axis_size(axis)
    low = range(start, size - 1, 2)
    return lax.ppermute(v, axis, [(i, i + 1) for i in low] + [(i + 1, i) for i in low])


def per_device(features, enc_weight, enc_bias, proj_weight, bottle_weight, bottle_bias, out_weight, dec_weight, dec_bias):
    first = (features, enc_weight.reshape(27, C, C), enc_bias.reshape(1, C))
    later = (
        dec_weight.reshape(27, C, C),
        dec_bias.reshape(1, C),
        bottle_weight.reshape(27 * 32, 512),
        proj_weight,
        out_weight,
        bottle_bias.reshape(1, 32),
    )
    ft, inner, outer, ew, eb = call(
        k_features,
        (S((18, C, 128), BF), S((2, C, 128), BF), S((2, C, 128), BF)) + tuple(S(v.shape, v.dtype) for v in first[1:]),
        *first,
        scratch=[pltpu.VMEM((C, 16, 128), BF), pltpu.VMEM((C * 16, 128), F32), pltpu.SemaphoreType.DMA((3,))],
        hbm=range(3),
    )
    outer, inner = swapped(outer, "sx", 1), swapped(inner, "sx", 0)
    we, wedge, be = call(
        k_enc_weights, (S((3 * C, 9 * C), BF), S((3 * C, 6 * C), BF), S((C, 128), F32)), ew, eb, flops=10**8
    )
    xh, fl, fr, inner, outer = call(k_faces, (S((4, C, 128), BF),) + (S((5, C, 128), BF),) * 4, inner, outer, ft)
    outer, inner = swapped(outer, "sy", 1), swapped(inner, "sy", 0)
    product, *later = call(
        k_interior,
        (S((20, 3 * C + 8, 128), F32),) + tuple(S(v.shape, v.dtype) for v in later),
        ft,
        xh,
        we,
        *later,
        scratch=[pltpu.VMEM((20, 9, C + 16, 128), BF), pltpu.SemaphoreType.DMA((6,))],
        flops=4 * 10**8,
        hbm=range(3, 9),
    )
    em, pooled = call(k_encode, (S((18, C, 128), BF), S((8, 128), F32)), product, inner, outer, wedge, be)
    p_outer, p_inner = swapped(pooled, "sx", 1), swapped(pooled, "sx", 0)
    wd, bd, vt, ow2, bb2, smat = call(
        k_weights,
        (
            S((3 * C, 9 * C), BF),
            S((C, 128), F32),
            S((C, 9 * 128), BF),
            S((C, 128), BF),
            S((1, C), F32),
            S((256, 9 * 128), BF),
        ),
        *later,
        flops=4 * 10**8,
    )
    d = call(
        k_decode,
        S((16, C, 128), F32),
        fl,
        fr,
        inner,
        outer,
        em,
        we,
        be,
        wd,
        bd,
        scratch=[pltpu.VMEM((18, 9, C + 16, 128), BF), pltpu.VMEM((18, 3 * C + 8, 128), F32)],
        flops=4 * 10**8,
    )
    message = call(k_message, S((NSY, 8, 128), F32), p_inner, pooled, p_outer, vt)
    everyone = lax.all_to_all(message, "sy", 0, 0, tiled=True)
    partial = call(k_bottleneck, S((NSY, 24, 128), BF), everyone, vt, bb2, ow2)
    parts = lax.all_to_all(partial, "sy", 0, 0, tiled=True)
    return call(
        k_final,
        S((C, 16, 128), BF),
        parts,
        smat,
        wd,
        d,
        scratch=[
            pltpu.VMEM((4, 9, C + 16, 128), BF),
            pltpu.VMEM((4, 3 * C + 8, 128), F32),
            pltpu.VMEM((4, 256, 128), F32),
            pltpu.VMEM((C, 16, 128), BF),
            pltpu.SemaphoreType.DMA((4,)),
        ],
        out_space=pltpu.HBM,
    )


def solution(mesh):
    in_specs = (P(None, "sx", "sy"), P(), P(), P(), P(None, None, None, "sy", None), P("sy"), P("sy", None), P(), P())

    return jax.shard_map(per_device, mesh=mesh, in_specs=in_specs, out_specs=P(None, "sx", "sy"), check_vma=False)
```

```python
import jax
import jax.numpy as jnp
from jax import lax
from jax.experimental import pallas as pl
from jax.experimental.pallas import tpu as pltpu
from jax.sharding import PartitionSpec as P


F32 = jnp.float32
BF = jnp.bfloat16
C = 64
NSX = 32
NSY = 16


def call(kernel, outs, *ins, scratch=(), flops=1000000, limit=16, hbm=(), out_space=pltpu.VMEM):
    ins = [pltpu.with_memory_space_constraint(v, pltpu.HBM) if i in hbm else v for i, v in enumerate(ins)]
    return pl.pallas_call(
        kernel,
        out_shape=outs,
        in_specs=[pl.BlockSpec(memory_space=pltpu.HBM if i in hbm else pltpu.VMEM) for i in range(len(ins))],
        out_specs=jax.tree.map(lambda _: pl.BlockSpec(memory_space=out_space), outs),
        scratch_shapes=list(scratch),
        compiler_params=pltpu.CompilerParams(vmem_limit_bytes=limit * 2**20),
        cost_estimate=pl.CostEstimate(flops=flops, transcendentals=0, bytes_accessed=100000),
    )(*ins)


def S(shape, dtype):
    return jax.ShapeDtypeStruct(shape, dtype)


def dot(a, b):
    return jnp.dot(a, b, preferred_element_type=F32)


def dot_nt(a, b):
    return lax.dot_general(a, b, (((1,), (1,)), ((), ())), preferred_element_type=F32)


def lanes_of(rows):
    return lax.broadcasted_iota(jnp.int32, (rows, 128), 1)


def roll(v, shift):
    shift = shift % 128
    return v if shift == 0 else pltpu.roll(v, shift, 1)


def even_of(axis):
    return lax.rem(lax.axis_index(axis), 2) == 0


def fetches(sources, targets, sem):
    copies = [pltpu.make_async_copy(a, b, sem.at[i]) for i, (a, b) in enumerate(zip(sources, targets))]
    for copy in copies:
        copy.start()
    return copies


def k_features(x_ref, ew_hbm, eb_hbm, ft_ref, inner_ref, outer_ref, ew_ref, eb_ref, held, buf, sem):
    copies = fetches((x_ref, ew_hbm, eb_hbm), (held, ew_ref, eb_ref), sem)
    even = even_of("sx")
    copies[0].wait()
    buf[...] = held[...].reshape(C * 16, 128).astype(F32)

    def row(x):
        return buf[pl.ds(x, C, stride=16), :]

    for k in range(2):
        low, high = row(k), row(14 + k)
        inner_ref[k] = jnp.where(even, high, low).astype(BF)
        outer_ref[k] = jnp.where(even, low, high).astype(BF)
    for x in range(16):
        ft_ref[x + 2] = row(x).astype(BF)
    for copy in copies[1:]:
        copy.wait()


def k_faces(pair_ref, outer_ref, ft_ref, x_ref, left_ref, right_ref, s_inner_ref, s_outer_ref):
    lane = lanes_of(C)
    even_x, even_y = even_of("sx"), even_of("sy")
    for k in range(2):
        inner, outer = jnp.where(even_x, pair_ref[1, k], pair_ref[0, k]), outer_ref[k]
        x_ref[k] = jnp.where(even_x, outer, inner)
        x_ref[2 + k] = jnp.where(even_x, inner, outer)
    for g in range(5):
        left = None
        for q in range(4):
            r = 4 * g + q
            v = x_ref[r] if r < 2 else ft_ref[r] if r < 18 else x_ref[r - 16]
            v = v.astype(F32)
            a, b = roll(v, 32 * q), roll(v, 32 * q - 96)
            if q == 0:
                left, right = a, b
            else:
                here = lane >= 32 * q
                left, right = jnp.where(here, a, left), jnp.where(here, b, right)
        left_ref[g] = left.astype(BF)
        right_ref[g] = right.astype(BF)
        s_inner_ref[g] = jnp.where(even_y, right, left).astype(BF)
        s_outer_ref[g] = jnp.where(even_y, left, right).astype(BF)


def arranged(w_ref, out_ref, taps):
    for a in range(3):
        for at in range(0, len(taps), 2):
            blocks = [w_ref[a * 9 + t] for t in taps[at : at + 2]]
            wide = blocks[0] if len(blocks) == 1 else jnp.concatenate(blocks, axis=1)
            out_ref[pl.ds(a * C, C), pl.ds(C * at, wide.shape[1])] = wide


def column(b_ref):
    row = jnp.broadcast_to(b_ref[...], (C, C))
    same = lax.broadcasted_iota(jnp.int32, (C, C), 0) == lax.broadcasted_iota(jnp.int32, (C, C), 1)
    return jnp.broadcast_to(jnp.sum(jnp.where(same, row, 0.0), axis=1, keepdims=True), (C, 128))


def interp_weight(g, cell, count, cells):
    num = 2 * g - 7
    low = jnp.right_shift(num, 4)
    w = (num - 16 * low).astype(F32) * (1.0 / 16.0)
    w = jnp.where((low < 0) | (low >= cells - 1), 0.0, w)
    low = jnp.clip(low, 0, cells - 1)
    value = jnp.where(cell == low, 1.0 - w, jnp.where(cell == low + 1, w, 0.0))
    return jnp.where((g >= 0) & (g < count), value, 0.0)


def k_enc_weights(ew, eb, we_ref, wedge_ref, be_ref):
    arranged(ew, we_ref, range(9))
    arranged(ew, wedge_ref, (0, 1, 2, 6, 7, 8))
    be_ref[...] = column(eb)


def k_weights(bw, proj, ow, bb, vt_ref, ow2_ref, bb2_ref):
    p = proj[...]
    r = dot_nt(bw[...], jnp.concatenate([p, p], axis=0))
    half = lanes_of(C) < C
    for ab in range(9):
        both = jnp.where(half, r[96 * ab : 96 * ab + 64], r[96 * ab + 32 : 96 * ab + 96])
        vt_ref[:, pl.ds(128 * ab, 128)] = both.astype(BF)
    o = ow[...]
    none = jnp.zeros_like(o)
    ow2_ref[...] = jnp.concatenate([jnp.concatenate([o, none], axis=1), jnp.concatenate([none, o], axis=1)], axis=0)
    bb2_ref[...] = jnp.concatenate([bb[...], bb[...]], axis=1)


def k_dec_weights(dw, db, wd_ref, bd_ref, s_ref):
    arranged(dw, wd_ref, range(9))
    bd_ref[...] = column(db)
    j = lax.axis_index("sy")
    row = lax.broadcasted_iota(jnp.int32, (32, 128), 0)
    lane = lax.broadcasted_iota(jnp.int32, (32, 128), 1)
    y, z = jnp.right_shift(lane, 4), jnp.bitwise_and(lane, 15)
    cell_y = j - 1 + jnp.right_shift(row, 3)
    zero = jnp.zeros((96, 128), BF)
    for b in range(3):
        wy = interp_weight(8 * j + y + (b - 1), cell_y, 8 * NSY, NSY)
        wy = jnp.where(row < 24, wy, 0.0)
        for c in range(3):
            for zo in range(2):
                wz = interp_weight(z + (c - 1), 1 - zo, 16, 2)
                at = pl.ds(128 * (3 * b + c), 128)
                s_ref[pl.ds(128 * zo, 32), at] = (wy * wz).astype(BF)
                s_ref[pl.ds(128 * zo + 32, 96), at] = zero


def taps_of(v, z):
    zero = jnp.zeros_like(v)
    return [jnp.where(z == 0, zero, roll(v, 1)), v, jnp.where(z == 15, zero, roll(v, -1))]


def put_taps(parts, xm, n, z):
    for b, v in enumerate(parts):
        for c, tap in enumerate(taps_of(v, z)):
            xm[n, 3 * b + c, pl.ds(0, C), :] = tap


def products(w_ref, xm, first, last, store):
    w = w_ref[...]

    def block(n):
        return jnp.concatenate([xm[n, t, pl.ds(0, C), :] for t in range(9)], axis=0)

    for n in range(first, last, 2):
        if n + 1 < last:
            g = dot(w, jnp.concatenate([block(n), block(n + 1)], axis=1))
            store(n, g[:, :128])
            store(n + 1, g[:, 128:])
        else:
            store(n, dot(w, block(n)))


def into(g_ref):
    def store(n, g):
        g_ref[n, pl.ds(0, 3 * C), :] = g

    return store


def summed(g_ref, r):
    return g_ref[r, pl.ds(0, C), :] + g_ref[r + 1, pl.ds(C, C), :] + g_ref[r + 2, pl.ds(2 * C, C), :]


def summed_packed(packed, g, lane):
    v = packed[g][:C]
    for a in (1, 2):
        this, after = packed[g][a * C : a * C + C], packed[min(g + 1, 4)][a * C : a * C + C]
        v = v + roll(jnp.where(lane < 32 * a, after, this), -32 * a)
    return v


def packed_products(w, blocks):
    out = []
    for n in range(0, 5, 2):
        if n + 1 < 5:
            g = dot(w, jnp.concatenate([blocks[n], blocks[n + 1]], axis=1))
            out += [g[:, :128], g[:, 128:]]
        else:
            out.append(dot(w, blocks[n]))
    return out


def y_halos(inner_ref, outer_ref, g):
    even_y = even_of("sy")
    inner, outer = inner_ref[g], outer_ref[g]
    return jnp.where(even_y, outer, inner), jnp.where(even_y, inner, outer)


def k_interior(ft_ref, x_ref, w_ref, *refs):
    sources, g_ref, targets, xm, sem = refs[:6], refs[6], refs[7:13], refs[13], refs[14]
    copies = fetches(sources, targets, sem)
    lane = lanes_of(C)
    z = jnp.bitwise_and(lane, 15)
    for r in range(20):
        v = x_ref[r] if r < 2 else ft_ref[r] if r < 18 else x_ref[r - 16]
        zero = jnp.zeros_like(v)
        put_taps(
            [jnp.where(lane < 16, zero, roll(v, 16)), v, jnp.where(lane >= 112, zero, roll(v, -16))], xm, r, z
        )
    products(w_ref, xm, 0, 20, into(g_ref))
    for copy in copies:
        copy.wait()


def k_encode(g_ref, inner_ref, outer_ref, w_ref, bias_ref, em_ref, pool_ref):
    lane = lanes_of(C)
    z = jnp.bitwise_and(lane, 15)
    even = jnp.bitwise_and(lane, 16) == 0
    edge = (lane < 16) | (lane >= 112)
    s = lax.axis_index("sx")
    blocks = []
    for g in range(5):
        hl, hr = y_halos(inner_ref, outer_ref, g)
        zero = jnp.zeros_like(hl)
        low, high = jnp.where(even, zero, hl), jnp.where(even, hr, zero)
        blocks.append(jnp.concatenate(taps_of(low, z) + taps_of(high, z), axis=0))
    packed = packed_products(w_ref[...], blocks)
    bias = bias_ref[...]
    best = [None, None]
    for r in range(18):
        if r % 4 == 0:
            at_edge = summed_packed(packed, r // 4, lane)
        v = summed(g_ref, r) + bias
        v = v + jnp.where(edge, roll(at_edge, -(32 * (r % 4) + 16)), 0.0)
        v = jnp.maximum(v, 0.0)
        if r == 0:
            v = jnp.where(s == 0, 0.0, v)
        if r == 17:
            v = jnp.where(s == NSX - 1, 0.0, v)
        em_ref[r] = v.astype(BF)
        if 1 <= r <= 16:
            cell = (r - 1) // 8
            best[cell] = v if best[cell] is None else jnp.maximum(best[cell], v)
    for cell in range(2):
        m = best[cell].astype(BF).astype(F32)
        for shift in (64, 32, 16, -1, -2, -4):
            m = jnp.maximum(m, roll(m, shift))
        best[cell] = m
    first = lane == 0
    both = [jnp.where(first, best[0], roll(best[1], 1)), jnp.where(first, roll(best[0], -8), roll(best[1], -7))]
    pool_ref[...] = jnp.transpose(jnp.concatenate(both, axis=0))[:8]


def k_decode(
    fl_ref, fr_ref, inner_ref, outer_ref, em_ref, we_ref, be_ref, w_ref, bias_ref, d_ref, xm, g_ref
):
    lane = lanes_of(C)
    z = jnp.bitwise_and(lane, 15)
    even = jnp.bitwise_and(lane, 16) == 0
    s, j = lax.axis_index("sx"), lax.axis_index("sy")
    blocks = []
    for g in range(5):
        hl, hr = y_halos(inner_ref, outer_ref, g)
        fl, fr = fl_ref[g], fr_ref[g]
        parts = [
            jnp.where(even, roll(fr, -16), roll(hl, 16)),
            jnp.where(even, hr, hl),
            jnp.where(even, roll(hr, -16), roll(fl, 16)),
        ]
        blocks.append(jnp.concatenate([tap for v in parts for tap in taps_of(v, z)], axis=0))
    packed = packed_products(we_ref[...], blocks)
    outside = (even & (j == NSY - 1)) | (~even & (j == 0))
    halo = []
    for g in range(5):
        v = summed_packed(packed, g, lane) + be_ref[...]
        v = jnp.where(outside, 0.0, jnp.maximum(v, 0.0))
        if g == 0:
            v = jnp.where((lane < 32) & (s == 0), 0.0, v)
        if g == 4:
            v = jnp.where((lane >= 64) | ((lane >= 32) & (s == NSX - 1)), 0.0, v)
        halo.append(v.astype(BF))
    for r in range(18):
        v = em_ref[r]
        beside = roll(halo[r // 4], -(32 * (r % 4) + 16))
        put_taps(
            [jnp.where(lane < 16, beside, roll(v, 16)), v, jnp.where(lane >= 112, beside, roll(v, -16))], xm, r, z
        )
    products(w_ref, xm, 0, 18, into(g_ref))
    bias = bias_ref[...]
    for x in range(16):
        d_ref[x] = summed(g_ref, x) + bias


def k_message(pair_ref, own_ref, outer_ref, out_ref):
    even = even_of("sx")
    inner, outer = jnp.where(even, pair_ref[1, 0:2], pair_ref[0, 0:2]), outer_ref[0:2]
    left, right = jnp.where(even, outer, inner), jnp.where(even, inner, outer)
    message = jnp.concatenate([left, own_ref[0:2], right, jnp.zeros((2, 128), F32)], axis=0)
    for i in range(NSY):
        out_ref[i] = message


def k_bottleneck(p_ref, vt_ref, bb_ref, ow_ref, out_ref):
    p = p_ref[...]
    pieces = []
    none = jnp.zeros((1, 8, 128), F32)
    for a in range(3):
        moved = p if a == 0 else jnp.concatenate([p[:, a:], p[:, :a]], axis=1)
        for b in range(3):
            if b == 0:
                v = jnp.concatenate([none, moved[:-1]], axis=0)
            elif b == 1:
                v = moved
            else:
                v = jnp.concatenate([moved[1:], none], axis=0)
            pieces.append(v.reshape(128, 128).astype(BF))
    h = dot_nt(jnp.concatenate(pieces, axis=1), vt_ref[...])
    h = jnp.maximum(h + bb_ref[...], 0.0).astype(BF)
    low = dot(h, ow_ref[...]).astype(BF).astype(F32)
    zero = jnp.zeros((8, 128), F32)
    for i in range(NSY):
        before = low[8 * (i - 1) : 8 * i] if i else zero
        after = low[8 * (i + 1) : 8 * (i + 2)] if i < NSY - 1 else zero
        out_ref[i] = jnp.concatenate([before, low[8 * i : 8 * i + 8], after], axis=0).astype(BF)


def k_final(parts_ref, s_ref, w_ref, d_ref, out_ref, xt, q_ref, buf, done, sem):
    total = parts_ref[0].astype(F32)
    for i in range(1, NSY):
        total = total + parts_ref[i].astype(F32)
    total = jnp.concatenate([total, jnp.zeros((104, 128), F32)], axis=0)
    lt = jnp.transpose(total)
    lane = lanes_of(C)
    left = []
    for cell in range(4):
        here = jnp.bitwise_and(lane, 7) == cell
        left.append(jnp.concatenate([jnp.where(here, lt[:C], 0.0), jnp.where(here, lt[C:], 0.0)], axis=1).astype(BF))
    t = dot(jnp.concatenate(left, axis=0), s_ref[...])
    for cell in range(4):
        for bc in range(9):
            xt[cell, bc, pl.ds(0, C), :] = t[C * cell : C * cell + C, 128 * bc : 128 * bc + 128].astype(BF)
    products(w_ref, xt, 0, 4, into(q_ref))
    s = lax.axis_index("sx")
    first, last = s == 0, s == NSX - 1
    copies = []
    for part in range(4):
        rows = 16
        for x in range(16):
            v = d_ref[x, pl.ds(rows * part, rows), :]
            for a in range(3):
                g = x + a - 1
                num = 2 * g - 7
                low = num // 16
                high = (num - 16 * low) / 16.0
                cell = low + 1
                w_low, w_high = jnp.float32(1.0 - high), jnp.float32(high)
                if cell == 0:
                    w_low = jnp.where(first, 0.0, w_low)
                    w_high = jnp.where(first, 0.0 if g < 0 else 1.0, w_high)
                if cell == 2:
                    w_low = jnp.where(last, 0.0 if g > 15 else 1.0, w_low)
                    w_high = jnp.where(last, 0.0, w_high)
                at = pl.ds(C * a + rows * part, rows)
                v = v + w_low * q_ref[cell, at, :]
                v = v + w_high * q_ref[cell + 1, at, :]
            buf[part, pl.ds(x, rows, stride=16), :] = v
        at = pl.ds(rows * part, rows)
        done[at] = buf[part].reshape(rows, 16, 128).astype(BF)
        copy = pltpu.make_async_copy(done.at[at], out_ref.at[at], sem.at[part])
        copy.start()
        copies.append(copy)
    for copy in copies:
        copy.wait()


def swapped(v, axis, start):
    size = lax.axis_size(axis)
    low = range(start, size - 1, 2)
    return lax.ppermute(v, axis, [(i, i + 1) for i in low] + [(i + 1, i) for i in low])


def paired(v, axis):
    pairs = [[i, i + 1] for i in range(0, lax.axis_size(axis), 2)]
    return lax.all_gather(v, axis, axis_index_groups=pairs)


def per_device(features, enc_weight, enc_bias, proj_weight, bottle_weight, bottle_bias, out_weight, dec_weight, dec_bias):
    first = (features, enc_weight.reshape(27, C, C), enc_bias.reshape(1, C))
    later = (
        dec_weight.reshape(27, C, C),
        dec_bias.reshape(1, C),
        bottle_weight.reshape(27 * 32, 512),
        proj_weight,
        out_weight,
        bottle_bias.reshape(1, 32),
    )
    ft, inner, outer, ew, eb = call(
        k_features,
        (S((18, C, 128), BF), S((2, C, 128), BF), S((2, C, 128), BF)) + tuple(S(v.shape, v.dtype) for v in first[1:]),
        *first,
        scratch=[pltpu.VMEM((C, 16, 128), BF), pltpu.VMEM((C * 16, 128), F32), pltpu.SemaphoreType.DMA((3,))],
        hbm=range(3),
    )
    outer, pair = swapped(outer, "sx", 1), paired(inner, "sx")
    we, wedge, be = call(
        k_enc_weights, (S((3 * C, 9 * C), BF), S((3 * C, 6 * C), BF), S((C, 128), F32)), ew, eb, flops=10**8
    )
    xh, fl, fr, inner, outer = call(k_faces, (S((4, C, 128), BF),) + (S((5, C, 128), BF),) * 4, pair, outer, ft)
    outer, inner = swapped(outer, "sy", 1), swapped(inner, "sy", 0)
    product, *later = call(
        k_interior,
        (S((20, 3 * C + 8, 128), F32),) + tuple(S(v.shape, v.dtype) for v in later),
        ft,
        xh,
        we,
        *later,
        scratch=[pltpu.VMEM((20, 9, C + 16, 128), BF), pltpu.SemaphoreType.DMA((6,))],
        flops=4 * 10**8,
        hbm=range(3, 9),
    )
    em, pooled = call(k_encode, (S((18, C, 128), BF), S((8, 128), F32)), product, inner, outer, wedge, be)
    p_outer, p_pair = swapped(pooled, "sx", 1), paired(pooled, "sx")
    vt, ow2, bb2 = call(k_weights, (S((C, 9 * 128), BF), S((C, 128), BF), S((1, C), F32)), *later[2:], flops=4 * 10**8)
    wd, bd, smat = call(
        k_dec_weights, (S((3 * C, 9 * C), BF), S((C, 128), F32), S((256, 9 * 128), BF)), *later[:2], flops=10**8
    )
    d = call(
        k_decode,
        S((16, C, 128), F32),
        fl,
        fr,
        inner,
        outer,
        em,
        we,
        be,
        wd,
        bd,
        scratch=[pltpu.VMEM((18, 9, C + 16, 128), BF), pltpu.VMEM((18, 3 * C + 8, 128), F32)],
        flops=4 * 10**8,
    )
    message = call(k_message, S((NSY, 8, 128), F32), p_pair, pooled, p_outer)
    everyone = lax.all_to_all(message, "sy", 0, 0, tiled=True)
    partial = call(k_bottleneck, S((NSY, 24, 128), BF), everyone, vt, bb2, ow2)
    parts = lax.all_to_all(partial, "sy", 0, 0, tiled=True)
    return call(
        k_final,
        S((C, 16, 128), BF),
        parts,
        smat,
        wd,
        d,
        scratch=[
            pltpu.VMEM((4, 9, C + 16, 128), BF),
            pltpu.VMEM((4, 3 * C + 8, 128), F32),
            pltpu.VMEM((4, 256, 128), F32),
            pltpu.VMEM((C, 16, 128), BF),
            pltpu.SemaphoreType.DMA((4,)),
        ],
        out_space=pltpu.HBM,
    )


def solution(mesh):
    in_specs = (P(None, "sx", "sy"), P(), P(), P(), P(None, None, None, "sy", None), P("sy"), P("sy", None), P(), P())

    return jax.shard_map(per_device, mesh=mesh, in_specs=in_specs, out_specs=P(None, "sx", "sy"), check_vma=False)
```

```python
import jax
import jax.numpy as jnp
from jax import lax
from jax.experimental import pallas as pl
from jax.experimental.pallas import tpu as pltpu
from jax.sharding import PartitionSpec as P


F32 = jnp.float32
BF = jnp.bfloat16
C = 64
NSX = 32
NSY = 16
STRIDE = 17


def call(kernel, outs, *ins, scratch=(), flops=1000000, limit=16, hbm=(), out_space=pltpu.VMEM):
    ins = [pltpu.with_memory_space_constraint(v, pltpu.HBM) if i in hbm else v for i, v in enumerate(ins)]
    return pl.pallas_call(
        kernel,
        out_shape=outs,
        in_specs=[pl.BlockSpec(memory_space=pltpu.HBM if i in hbm else pltpu.VMEM) for i in range(len(ins))],
        out_specs=jax.tree.map(lambda _: pl.BlockSpec(memory_space=out_space), outs),
        scratch_shapes=list(scratch),
        compiler_params=pltpu.CompilerParams(vmem_limit_bytes=limit * 2**20),
        cost_estimate=pl.CostEstimate(flops=flops, transcendentals=0, bytes_accessed=100000),
    )(*ins)


def S(shape, dtype):
    return jax.ShapeDtypeStruct(shape, dtype)


def dot(a, b):
    return jnp.dot(a, b, preferred_element_type=F32)


def dot_nt(a, b):
    return lax.dot_general(a, b, (((1,), (1,)), ((), ())), preferred_element_type=F32)


def lanes_of(rows):
    return lax.broadcasted_iota(jnp.int32, (rows, 128), 1)


def roll(v, shift):
    shift = shift % 128
    return v if shift == 0 else pltpu.roll(v, shift, 1)


def even_of(axis):
    return lax.rem(lax.axis_index(axis), 2) == 0


def fetches(sources, targets, sem):
    copies = [pltpu.make_async_copy(a, b, sem.at[i]) for i, (a, b) in enumerate(zip(sources, targets))]
    for copy in copies:
        copy.start()
    return copies


def k_features(x_ref, ew_hbm, eb_hbm, ft_ref, inner_ref, outer_ref, ew_ref, eb_ref, held, buf, sem):
    copies = fetches((x_ref, ew_hbm, eb_hbm), (held, ew_ref, eb_ref), sem)
    even = even_of("sx")
    copies[0].wait()
    for c in range(C):
        buf[pl.ds(STRIDE * c, 16), :] = held[c].astype(F32)

    def row(x):
        return buf[pl.ds(x, C, stride=STRIDE), :]

    for k in range(2):
        low, high = row(k), row(14 + k)
        inner_ref[k] = jnp.where(even, high, low).astype(BF)
        outer_ref[k] = jnp.where(even, low, high).astype(BF)
    for x in range(16):
        ft_ref[x + 2] = row(x).astype(BF)
    for copy in copies[1:]:
        copy.wait()


def k_faces(pair_ref, outer_ref, ft_ref, x_ref, left_ref, right_ref, s_inner_ref, s_outer_ref):
    lane = lanes_of(C)
    even_x, even_y = even_of("sx"), even_of("sy")
    for k in range(2):
        inner, outer = jnp.where(even_x, pair_ref[1, k], pair_ref[0, k]), outer_ref[k]
        x_ref[k] = jnp.where(even_x, outer, inner)
        x_ref[2 + k] = jnp.where(even_x, inner, outer)
    for g in range(5):
        left = None
        for q in range(4):
            r = 4 * g + q
            v = x_ref[r] if r < 2 else ft_ref[r] if r < 18 else x_ref[r - 16]
            v = v.astype(F32)
            a, b = roll(v, 32 * q), roll(v, 32 * q - 96)
            if q == 0:
                left, right = a, b
            else:
                here = lane >= 32 * q
                left, right = jnp.where(here, a, left), jnp.where(here, b, right)
        left_ref[g] = left.astype(BF)
        right_ref[g] = right.astype(BF)
        s_inner_ref[g] = jnp.where(even_y, right, left).astype(BF)
        s_outer_ref[g] = jnp.where(even_y, left, right).astype(BF)


def arranged(w_ref, out_ref, taps):
    for a in range(3):
        for at in range(0, len(taps), 2):
            blocks = [w_ref[a * 9 + t] for t in taps[at : at + 2]]
            wide = blocks[0] if len(blocks) == 1 else jnp.concatenate(blocks, axis=1)
            out_ref[pl.ds(a * C, C), pl.ds(C * at, wide.shape[1])] = wide


def column(b_ref):
    row = jnp.broadcast_to(b_ref[...], (C, C))
    same = lax.broadcasted_iota(jnp.int32, (C, C), 0) == lax.broadcasted_iota(jnp.int32, (C, C), 1)
    return jnp.broadcast_to(jnp.sum(jnp.where(same, row, 0.0), axis=1, keepdims=True), (C, 128))


def interp_weight(g, cell, count, cells):
    num = 2 * g - 7
    low = jnp.right_shift(num, 4)
    w = (num - 16 * low).astype(F32) * (1.0 / 16.0)
    w = jnp.where((low < 0) | (low >= cells - 1), 0.0, w)
    low = jnp.clip(low, 0, cells - 1)
    value = jnp.where(cell == low, 1.0 - w, jnp.where(cell == low + 1, w, 0.0))
    return jnp.where((g >= 0) & (g < count), value, 0.0)


def k_enc_weights(ew, eb, we_ref, wedge_ref, be_ref):
    arranged(ew, we_ref, range(9))
    arranged(ew, wedge_ref, (0, 1, 2, 6, 7, 8))
    be_ref[...] = column(eb)


def k_weights(bw, proj, ow, bb, vt_ref, ow2_ref, bb2_ref):
    p = proj[...]
    r = dot_nt(bw[...], jnp.concatenate([p, p], axis=0))
    half = lanes_of(C) < C
    for ab in range(9):
        both = jnp.where(half, r[96 * ab : 96 * ab + 64], r[96 * ab + 32 : 96 * ab + 96])
        vt_ref[:, pl.ds(128 * ab, 128)] = both.astype(BF)
    o = ow[...]
    none = jnp.zeros_like(o)
    ow2_ref[...] = jnp.concatenate([jnp.concatenate([o, none], axis=1), jnp.concatenate([none, o], axis=1)], axis=0)
    bb2_ref[...] = jnp.concatenate([bb[...], bb[...]], axis=1)


def k_dec_weights(dw_hbm, db_hbm, wd_ref, bd_ref, s_ref, dw, db, sem):
    copies = fetches((dw_hbm, db_hbm), (dw, db), sem)
    j = lax.axis_index("sy")
    row = lax.broadcasted_iota(jnp.int32, (16, 128), 0)
    lane = lax.broadcasted_iota(jnp.int32, (16, 128), 1)
    y, z = jnp.right_shift(lane, 4), jnp.bitwise_and(lane, 15)
    cell_y = j - 1 + jnp.right_shift(row, 2)
    zero = jnp.zeros((112, 128), BF)
    for b in range(3):
        wy = interp_weight(8 * j + y + (b - 1), cell_y, 8 * NSY, NSY)
        wy = jnp.where(row < 12, wy, 0.0)
        for c in range(3):
            for zo in range(2):
                wz = interp_weight(z + (c - 1), 1 - zo, 16, 2)
                at = pl.ds(128 * (3 * b + c), 128)
                s_ref[pl.ds(128 * zo, 16), at] = (wy * wz).astype(BF)
                s_ref[pl.ds(128 * zo + 16, 112), at] = zero
    for copy in copies:
        copy.wait()
    arranged(dw, wd_ref, range(9))
    bd_ref[...] = column(db)


def taps_of(v, z):
    zero = jnp.zeros_like(v)
    return [jnp.where(z == 0, zero, roll(v, 1)), v, jnp.where(z == 15, zero, roll(v, -1))]


def put_taps(parts, xm, n, z):
    for b, v in enumerate(parts):
        for c, tap in enumerate(taps_of(v, z)):
            xm[n, 3 * b + c, pl.ds(0, C), :] = tap


def products(w_ref, xm, first, last, store):
    w = w_ref[...]

    def block(n):
        return jnp.concatenate([xm[n, t, pl.ds(0, C), :] for t in range(9)], axis=0)

    for n in range(first, last, 2):
        if n + 1 < last:
            g = dot(w, jnp.concatenate([block(n), block(n + 1)], axis=1))
            store(n, g[:, :128])
            store(n + 1, g[:, 128:])
        else:
            store(n, dot(w, block(n)))


def into(g_ref):
    def store(n, g):
        g_ref[n, pl.ds(0, 3 * C), :] = g

    return store


def summed(g_ref, r):
    return g_ref[r, pl.ds(0, C), :] + g_ref[r + 1, pl.ds(C, C), :] + g_ref[r + 2, pl.ds(2 * C, C), :]


def summed_packed(packed, g, lane):
    v = packed[g][:C]
    for a in (1, 2):
        this, after = packed[g][a * C : a * C + C], packed[min(g + 1, 4)][a * C : a * C + C]
        v = v + roll(jnp.where(lane < 32 * a, after, this), -32 * a)
    return v


def packed_products(w, blocks):
    out = []
    for n in range(0, 5, 2):
        if n + 1 < 5:
            g = dot(w, jnp.concatenate([blocks[n], blocks[n + 1]], axis=1))
            out += [g[:, :128], g[:, 128:]]
        else:
            out.append(dot(w, blocks[n]))
    return out


def y_halos(inner_ref, outer_ref, g):
    even_y = even_of("sy")
    inner, outer = inner_ref[g], outer_ref[g]
    return jnp.where(even_y, outer, inner), jnp.where(even_y, inner, outer)


def k_interior(ft_ref, x_ref, w_ref, *refs):
    sources, g_ref, targets, xm, sem = refs[:4], refs[4], refs[5:9], refs[9], refs[10]
    copies = fetches(sources, targets, sem)
    lane = lanes_of(C)
    z = jnp.bitwise_and(lane, 15)
    for r in range(20):
        v = x_ref[r] if r < 2 else ft_ref[r] if r < 18 else x_ref[r - 16]
        zero = jnp.zeros_like(v)
        put_taps(
            [jnp.where(lane < 16, zero, roll(v, 16)), v, jnp.where(lane >= 112, zero, roll(v, -16))], xm, r, z
        )
    products(w_ref, xm, 0, 20, into(g_ref))
    for copy in copies:
        copy.wait()


def k_encode(g_ref, inner_ref, outer_ref, w_ref, bias_ref, em_ref, pool_ref):
    lane = lanes_of(C)
    z = jnp.bitwise_and(lane, 15)
    even = jnp.bitwise_and(lane, 16) == 0
    edge = (lane < 16) | (lane >= 112)
    s = lax.axis_index("sx")
    blocks = []
    for g in range(5):
        hl, hr = y_halos(inner_ref, outer_ref, g)
        zero = jnp.zeros_like(hl)
        low, high = jnp.where(even, zero, hl), jnp.where(even, hr, zero)
        blocks.append(jnp.concatenate(taps_of(low, z) + taps_of(high, z), axis=0))
    packed = packed_products(w_ref[...], blocks)
    bias = bias_ref[...]
    best = [None, None]
    for r in range(18):
        if r % 4 == 0:
            at_edge = summed_packed(packed, r // 4, lane)
        v = summed(g_ref, r) + bias
        v = v + jnp.where(edge, roll(at_edge, -(32 * (r % 4) + 16)), 0.0)
        v = jnp.maximum(v, 0.0)
        if r == 0:
            v = jnp.where(s == 0, 0.0, v)
        if r == 17:
            v = jnp.where(s == NSX - 1, 0.0, v)
        em_ref[r] = v.astype(BF)
        if 1 <= r <= 16:
            cell = (r - 1) // 8
            best[cell] = v if best[cell] is None else jnp.maximum(best[cell], v)
    halves = [jnp.maximum(m, roll(m, 64)) for m in best]
    m = jnp.where(lane < 64, halves[0], halves[1])
    for shift in (-32, -16, -1, -2, -4):
        m = jnp.maximum(m, roll(m, shift))
    m = jnp.transpose(m.astype(BF).astype(F32))
    rows = [jnp.concatenate([m[64 * x : 64 * x + 1], m[64 * x + 8 : 64 * x + 9]], axis=1) for x in range(2)]
    pool_ref[...] = jnp.concatenate(rows + [jnp.zeros((6, 128), F32)], axis=0)


def k_decode(
    fl_ref, fr_ref, inner_ref, outer_ref, em_ref, we_ref, be_ref, w_ref, bias_ref, d_ref, xm, g_ref
):
    lane = lanes_of(C)
    z = jnp.bitwise_and(lane, 15)
    even = jnp.bitwise_and(lane, 16) == 0
    s, j = lax.axis_index("sx"), lax.axis_index("sy")
    blocks = []
    for g in range(5):
        hl, hr = y_halos(inner_ref, outer_ref, g)
        fl, fr = fl_ref[g], fr_ref[g]
        parts = [
            jnp.where(even, roll(fr, -16), roll(hl, 16)),
            jnp.where(even, hr, hl),
            jnp.where(even, roll(hr, -16), roll(fl, 16)),
        ]
        blocks.append(jnp.concatenate([tap for v in parts for tap in taps_of(v, z)], axis=0))
    packed = packed_products(we_ref[...], blocks)
    outside = (even & (j == NSY - 1)) | (~even & (j == 0))
    halo = []
    for g in range(5):
        v = summed_packed(packed, g, lane) + be_ref[...]
        v = jnp.where(outside, 0.0, jnp.maximum(v, 0.0))
        if g == 0:
            v = jnp.where((lane < 32) & (s == 0), 0.0, v)
        if g == 4:
            v = jnp.where((lane >= 64) | ((lane >= 32) & (s == NSX - 1)), 0.0, v)
        halo.append(v.astype(BF))
    for r in range(18):
        v = em_ref[r]
        beside = roll(halo[r // 4], -(32 * (r % 4) + 16))
        put_taps(
            [jnp.where(lane < 16, beside, roll(v, 16)), v, jnp.where(lane >= 112, beside, roll(v, -16))], xm, r, z
        )
    products(w_ref, xm, 0, 18, into(g_ref))
    bias = bias_ref[...]
    for x in range(16):
        d_ref[x] = summed(g_ref, x) + bias


def k_message(pair_ref, own_ref, outer_ref, out_ref):
    even = even_of("sx")
    inner, outer = jnp.where(even, pair_ref[1, 0:2], pair_ref[0, 0:2]), outer_ref[0:2]
    left, right = jnp.where(even, outer, inner), jnp.where(even, inner, outer)
    message = jnp.concatenate([left, own_ref[0:2], right, jnp.zeros((2, 128), F32)], axis=0)
    message = message.astype(BF)
    for i in range(NSY):
        out_ref[i] = message


def k_bottleneck(p_ref, vt_ref, bb_ref, ow_ref, out_ref):
    p = p_ref[...].astype(F32)
    pieces = []
    none = jnp.zeros((1, 8, 128), F32)
    for a in range(3):
        moved = p if a == 0 else jnp.concatenate([p[:, a:], p[:, :a]], axis=1)
        for b in range(3):
            if b == 0:
                v = jnp.concatenate([none, moved[:-1]], axis=0)
            elif b == 1:
                v = moved
            else:
                v = jnp.concatenate([moved[1:], none], axis=0)
            pieces.append(v.reshape(128, 128).astype(BF))
    h = dot_nt(jnp.concatenate(pieces, axis=1), vt_ref[...])
    h = jnp.maximum(h + bb_ref[...], 0.0).astype(BF)
    low = dot(h, ow_ref[...])
    zero = jnp.zeros((4, 128), F32)
    rows = [zero] + [low[8 * i : 8 * i + 4] for i in range(NSY)] + [zero, zero]
    for i in range(NSY):
        out_ref[i] = jnp.concatenate(rows[i : i + 3] + [zero], axis=0).astype(BF)


def k_final(parts_ref, s_ref, w_ref, d_ref, out_ref, xt, q_ref, buf, done, sem):
    total = parts_ref[0].astype(F32)
    for i in range(1, NSY):
        total = total + parts_ref[i].astype(F32)
    total = jnp.concatenate([total, jnp.zeros((112, 128), F32)], axis=0)
    lt = jnp.transpose(total)
    lane = lanes_of(C)
    left = []
    for cell in range(4):
        here = jnp.bitwise_and(lane, 3) == cell
        left.append(jnp.concatenate([jnp.where(here, lt[:C], 0.0), jnp.where(here, lt[C:], 0.0)], axis=1).astype(BF))
    t = dot(jnp.concatenate(left, axis=0), s_ref[...])
    for cell in range(4):
        for bc in range(9):
            xt[cell, bc, pl.ds(0, C), :] = t[C * cell : C * cell + C, 128 * bc : 128 * bc + 128].astype(BF)
    products(w_ref, xt, 0, 4, into(q_ref))
    s = lax.axis_index("sx")
    first, last = s == 0, s == NSX - 1
    copies = []
    for part in range(4):
        rows = 16
        for x in range(16):
            v = d_ref[x, pl.ds(rows * part, rows), :]
            for a in range(3):
                g = x + a - 1
                num = 2 * g - 7
                low = num // 16
                high = (num - 16 * low) / 16.0
                cell = low + 1
                w_low, w_high = jnp.float32(1.0 - high), jnp.float32(high)
                if cell == 0:
                    w_low = jnp.where(first, 0.0, w_low)
                    w_high = jnp.where(first, 0.0 if g < 0 else 1.0, w_high)
                if cell == 2:
                    w_low = jnp.where(last, 0.0 if g > 15 else 1.0, w_low)
                    w_high = jnp.where(last, 0.0, w_high)
                at = pl.ds(C * a + rows * part, rows)
                v = v + w_low * q_ref[cell, at, :]
                v = v + w_high * q_ref[cell + 1, at, :]
            buf[part, pl.ds(x, rows, stride=STRIDE), :] = v
        at = pl.ds(rows * part, rows)
        for o in range(rows):
            done[rows * part + o] = buf[part, pl.ds(STRIDE * o, 16), :].astype(BF)
        copy = pltpu.make_async_copy(done.at[at], out_ref.at[at], sem.at[part])
        copy.start()
        copies.append(copy)
    for copy in copies:
        copy.wait()


def swapped(v, axis, start):
    size = lax.axis_size(axis)
    low = range(start, size - 1, 2)
    return lax.ppermute(v, axis, [(i, i + 1) for i in low] + [(i + 1, i) for i in low])


def paired(v, axis):
    pairs = [[i, i + 1] for i in range(0, lax.axis_size(axis), 2)]
    return lax.all_gather(v, axis, axis_index_groups=pairs)


def per_device(features, enc_weight, enc_bias, proj_weight, bottle_weight, bottle_bias, out_weight, dec_weight, dec_bias):
    first = (features, enc_weight.reshape(27, C, C), enc_bias.reshape(1, C))
    deep = (bottle_weight.reshape(27 * 32, 512), proj_weight, out_weight, bottle_bias.reshape(1, 32))
    last = (dec_weight.reshape(27, C, C), dec_bias.reshape(1, C))
    ft, inner, outer, ew, eb = call(
        k_features,
        (S((18, C, 128), BF), S((2, C, 128), BF), S((2, C, 128), BF)) + tuple(S(v.shape, v.dtype) for v in first[1:]),
        *first,
        scratch=[pltpu.VMEM((C, 16, 128), BF), pltpu.VMEM((C * STRIDE, 128), F32), pltpu.SemaphoreType.DMA((3,))],
        hbm=range(3),
    )
    outer, pair = swapped(outer, "sx", 1), paired(inner, "sx")
    we, wedge, be = call(
        k_enc_weights, (S((3 * C, 9 * C), BF), S((3 * C, 6 * C), BF), S((C, 128), F32)), ew, eb, flops=10**8
    )
    xh, fl, fr, inner, outer = call(k_faces, (S((4, C, 128), BF),) + (S((5, C, 128), BF),) * 4, pair, outer, ft)
    outer, inner = swapped(outer, "sy", 1), swapped(inner, "sy", 0)
    product, *deep = call(
        k_interior,
        (S((20, 3 * C + 8, 128), F32),) + tuple(S(v.shape, v.dtype) for v in deep),
        ft,
        xh,
        we,
        *deep,
        scratch=[pltpu.VMEM((20, 9, C + 16, 128), BF), pltpu.SemaphoreType.DMA((4,))],
        flops=4 * 10**8,
        hbm=range(3, 7),
    )
    em, pooled = call(k_encode, (S((18, C, 128), BF), S((8, 128), F32)), product, inner, outer, wedge, be)
    p_outer, p_pair = swapped(pooled, "sx", 1), paired(pooled, "sx")
    vt, ow2, bb2 = call(k_weights, (S((C, 9 * 128), BF), S((C, 128), BF), S((1, C), F32)), *deep, flops=4 * 10**8)
    wd, bd, smat = call(
        k_dec_weights,
        (S((3 * C, 9 * C), BF), S((C, 128), F32), S((256, 9 * 128), BF)),
        *last,
        scratch=[pltpu.VMEM(v.shape, v.dtype) for v in last] + [pltpu.SemaphoreType.DMA((2,))],
        flops=10**8,
        hbm=(0, 1),
    )
    d = call(
        k_decode,
        S((16, C, 128), F32),
        fl,
        fr,
        inner,
        outer,
        em,
        we,
        be,
        wd,
        bd,
        scratch=[pltpu.VMEM((18, 9, C + 16, 128), BF), pltpu.VMEM((18, 3 * C + 8, 128), F32)],
        flops=4 * 10**8,
    )
    message = call(k_message, S((NSY, 8, 128), BF), p_pair, pooled, p_outer)
    everyone = lax.all_to_all(message, "sy", 0, 0, tiled=True)
    partial = call(k_bottleneck, S((NSY, 16, 128), BF), everyone, vt, bb2, ow2)
    parts = lax.all_to_all(partial, "sy", 0, 0, tiled=True)
    return call(
        k_final,
        S((C, 16, 128), BF),
        parts,
        smat,
        wd,
        d,
        scratch=[
            pltpu.VMEM((4, 9, C + 16, 128), BF),
            pltpu.VMEM((4, 3 * C + 8, 128), F32),
            pltpu.VMEM((4, 16 * STRIDE, 128), F32),
            pltpu.VMEM((C, 16, 128), BF),
            pltpu.SemaphoreType.DMA((4,)),
        ],
        out_space=pltpu.HBM,
    )


def solution(mesh):
    in_specs = (P(None, "sx", "sy"), P(), P(), P(), P(None, None, None, "sy", None), P("sy"), P("sy", None), P(), P())

    return jax.shard_map(per_device, mesh=mesh, in_specs=in_specs, out_specs=P(None, "sx", "sy"), check_vma=False)
```

```python
import jax
import jax.numpy as jnp
from jax import lax
from jax.experimental import pallas as pl
from jax.experimental.pallas import tpu as pltpu
from jax.sharding import PartitionSpec as P


F32 = jnp.float32
BF = jnp.bfloat16
C = 64
NSX = 32
NSY = 16
STRIDE = 17


def call(kernel, outs, *ins, scratch=(), flops=1000000, limit=16, hbm=(), out_space=pltpu.VMEM):
    ins = [pltpu.with_memory_space_constraint(v, pltpu.HBM) if i in hbm else v for i, v in enumerate(ins)]
    return pl.pallas_call(
        kernel,
        out_shape=outs,
        in_specs=[pl.BlockSpec(memory_space=pltpu.HBM if i in hbm else pltpu.VMEM) for i in range(len(ins))],
        out_specs=jax.tree.map(lambda _: pl.BlockSpec(memory_space=out_space), outs),
        scratch_shapes=list(scratch),
        compiler_params=pltpu.CompilerParams(vmem_limit_bytes=limit * 2**20),
        cost_estimate=pl.CostEstimate(flops=flops, transcendentals=0, bytes_accessed=100000),
    )(*ins)


def S(shape, dtype):
    return jax.ShapeDtypeStruct(shape, dtype)


def dot(a, b):
    return jnp.dot(a, b, preferred_element_type=F32)


def dot_nt(a, b):
    return lax.dot_general(a, b, (((1,), (1,)), ((), ())), preferred_element_type=F32)


def lanes_of(rows):
    return lax.broadcasted_iota(jnp.int32, (rows, 128), 1)


def roll(v, shift):
    shift = shift % 128
    return v if shift == 0 else pltpu.roll(v, shift, 1)


def even_of(axis):
    return lax.rem(lax.axis_index(axis), 2) == 0


def fetches(sources, targets, sem):
    copies = [pltpu.make_async_copy(a, b, sem.at[i]) for i, (a, b) in enumerate(zip(sources, targets))]
    for copy in copies:
        copy.start()
    return copies


def k_features(x_ref, ew_hbm, eb_hbm, ft_ref, inner_ref, outer_ref, ew_ref, eb_ref, held, buf, sem):
    copies = fetches((x_ref, ew_hbm, eb_hbm), (held, ew_ref, eb_ref), sem)
    even = even_of("sx")
    copies[0].wait()
    for c in range(C):
        buf[pl.ds(STRIDE * c, 16), :] = held[c].astype(F32)

    def row(x):
        return buf[pl.ds(x, C, stride=STRIDE), :]

    for k in range(2):
        low, high = row(k), row(14 + k)
        inner_ref[k] = jnp.where(even, high, low).astype(BF)
        outer_ref[k] = jnp.where(even, low, high).astype(BF)
    for x in range(16):
        ft_ref[x + 2] = row(x).astype(BF)
    for copy in copies[1:]:
        copy.wait()


def k_faces(pair_ref, outer_ref, ft_ref, x_ref, left_ref, right_ref, s_inner_ref, s_outer_ref):
    lane = lanes_of(C)
    even_x, even_y = even_of("sx"), even_of("sy")
    for k in range(2):
        inner, outer = jnp.where(even_x, pair_ref[1, k], pair_ref[0, k]), outer_ref[k]
        x_ref[k] = jnp.where(even_x, outer, inner)
        x_ref[2 + k] = jnp.where(even_x, inner, outer)
    for g in range(5):
        left = None
        for q in range(4):
            r = 5 * q + g
            v = x_ref[r] if r < 2 else ft_ref[r] if r < 18 else x_ref[r - 16]
            v = v.astype(F32)
            a, b = roll(v, 32 * q), roll(v, 32 * q - 96)
            if q == 0:
                left, right = a, b
            else:
                here = lane >= 32 * q
                left, right = jnp.where(here, a, left), jnp.where(here, b, right)
        left_ref[g] = left.astype(BF)
        right_ref[g] = right.astype(BF)
        s_inner_ref[g] = jnp.where(even_y, right, left).astype(BF)
        s_outer_ref[g] = jnp.where(even_y, left, right).astype(BF)


def arranged(w_ref, out_ref, taps):
    for a in range(3):
        for at in range(0, len(taps), 2):
            blocks = [w_ref[a * 9 + t] for t in taps[at : at + 2]]
            wide = blocks[0] if len(blocks) == 1 else jnp.concatenate(blocks, axis=1)
            out_ref[pl.ds(a * C, C), pl.ds(C * at, wide.shape[1])] = wide


def column(b_ref):
    row = jnp.broadcast_to(b_ref[...], (C, C))
    same = lax.broadcasted_iota(jnp.int32, (C, C), 0) == lax.broadcasted_iota(jnp.int32, (C, C), 1)
    return jnp.broadcast_to(jnp.sum(jnp.where(same, row, 0.0), axis=1, keepdims=True), (C, 128))


def interp_weight(g, cell, count, cells):
    num = 2 * g - 7
    low = jnp.right_shift(num, 4)
    w = (num - 16 * low).astype(F32) * (1.0 / 16.0)
    w = jnp.where((low < 0) | (low >= cells - 1), 0.0, w)
    low = jnp.clip(low, 0, cells - 1)
    value = jnp.where(cell == low, 1.0 - w, jnp.where(cell == low + 1, w, 0.0))
    return jnp.where((g >= 0) & (g < count), value, 0.0)


def k_enc_weights(ew, eb, we_ref, wedge_ref, be_ref):
    arranged(ew, we_ref, range(9))
    arranged(ew, wedge_ref, (0, 1, 2, 6, 7, 8))
    be_ref[...] = column(eb)


def k_weights(bw, proj, ow, bb, vt_ref, ow2_ref, bb2_ref):
    p = proj[...]
    r = dot_nt(bw[...], jnp.concatenate([p, p], axis=0))
    half = lanes_of(C) < C
    for ab in range(9):
        both = jnp.where(half, r[96 * ab : 96 * ab + 64], r[96 * ab + 32 : 96 * ab + 96])
        vt_ref[:, pl.ds(128 * ab, 128)] = both.astype(BF)
    o = ow[...]
    none = jnp.zeros_like(o)
    ow2_ref[...] = jnp.concatenate([jnp.concatenate([o, none], axis=1), jnp.concatenate([none, o], axis=1)], axis=0)
    bb2_ref[...] = jnp.concatenate([bb[...], bb[...]], axis=1)


def k_dec_weights(dw_hbm, db_hbm, wd_ref, bd_ref, s_ref, dw, db, sem):
    copies = fetches((dw_hbm, db_hbm), (dw, db), sem)
    j = lax.axis_index("sy")
    row = lax.broadcasted_iota(jnp.int32, (16, 128), 0)
    lane = lax.broadcasted_iota(jnp.int32, (16, 128), 1)
    y, z = jnp.right_shift(lane, 4), jnp.bitwise_and(lane, 15)
    cell_y = j - 1 + jnp.right_shift(row, 2)
    zero = jnp.zeros((112, 128), BF)
    for b in range(3):
        wy = interp_weight(8 * j + y + (b - 1), cell_y, 8 * NSY, NSY)
        wy = jnp.where(row < 12, wy, 0.0)
        for c in range(3):
            for zo in range(2):
                wz = interp_weight(z + (c - 1), 1 - zo, 16, 2)
                at = pl.ds(128 * (3 * b + c), 128)
                s_ref[pl.ds(128 * zo, 16), at] = (wy * wz).astype(BF)
                s_ref[pl.ds(128 * zo + 16, 112), at] = zero
    for copy in copies:
        copy.wait()
    arranged(dw, wd_ref, range(9))
    bd_ref[...] = column(db)


def taps_of(v, z):
    zero = jnp.zeros_like(v)
    return [jnp.where(z == 0, zero, roll(v, 1)), v, jnp.where(z == 15, zero, roll(v, -1))]


def put_taps(parts, xm, n, z):
    for b, v in enumerate(parts):
        for c, tap in enumerate(taps_of(v, z)):
            xm[n, 3 * b + c, pl.ds(0, C), :] = tap


def products(w_ref, xm, first, last, store):
    w = w_ref[...]

    def block(n):
        return jnp.concatenate([xm[n, t, pl.ds(0, C), :] for t in range(9)], axis=0)

    for n in range(first, last, 2):
        if n + 1 < last:
            g = dot(w, jnp.concatenate([block(n), block(n + 1)], axis=1))
            store(n, g[:, :128])
            store(n + 1, g[:, 128:])
        else:
            store(n, dot(w, block(n)))


def into(g_ref):
    def store(n, g):
        g_ref[n, pl.ds(0, 3 * C), :] = g

    return store


def summed(g_ref, r):
    return g_ref[r, pl.ds(0, C), :] + g_ref[r + 1, pl.ds(C, C), :] + g_ref[r + 2, pl.ds(2 * C, C), :]


def summed_packed(packed, g):
    v = packed[g][:C]
    for a in (1, 2):
        tap = packed[(g + a) % 5][a * C : a * C + C]
        v = v + (tap if g + a < 5 else roll(tap, -32))
    return v


def packed_products(w, blocks):
    out = []
    for n in range(0, 5, 2):
        if n + 1 < 5:
            g = dot(w, jnp.concatenate([blocks[n], blocks[n + 1]], axis=1))
            out += [g[:, :128], g[:, 128:]]
        else:
            out.append(dot(w, blocks[n]))
    return out


def y_halos(inner_ref, outer_ref, g):
    even_y = even_of("sy")
    inner, outer = inner_ref[g], outer_ref[g]
    return jnp.where(even_y, outer, inner), jnp.where(even_y, inner, outer)


def k_interior(ft_ref, x_ref, w_ref, *refs):
    sources, g_ref, targets, xm, sem = refs[:4], refs[4], refs[5:9], refs[9], refs[10]
    copies = fetches(sources, targets, sem)
    lane = lanes_of(C)
    z = jnp.bitwise_and(lane, 15)
    for r in range(20):
        v = x_ref[r] if r < 2 else ft_ref[r] if r < 18 else x_ref[r - 16]
        zero = jnp.zeros_like(v)
        put_taps(
            [jnp.where(lane < 16, zero, roll(v, 16)), v, jnp.where(lane >= 112, zero, roll(v, -16))], xm, r, z
        )
    products(w_ref, xm, 0, 20, into(g_ref))
    for copy in copies:
        copy.wait()


def k_encode(g_ref, inner_ref, outer_ref, w_ref, bias_ref, em_ref, pool_ref):
    lane = lanes_of(C)
    z = jnp.bitwise_and(lane, 15)
    even = jnp.bitwise_and(lane, 16) == 0
    edge = (lane < 16) | (lane >= 112)
    s = lax.axis_index("sx")
    blocks = []
    for g in range(5):
        hl, hr = y_halos(inner_ref, outer_ref, g)
        zero = jnp.zeros_like(hl)
        low, high = jnp.where(even, zero, hl), jnp.where(even, hr, zero)
        blocks.append(jnp.concatenate(taps_of(low, z) + taps_of(high, z), axis=0))
    packed = packed_products(w_ref[...], blocks)
    bias = bias_ref[...]
    best = [None, None]
    at_edge = [summed_packed(packed, g) for g in range(5)]
    for r in range(18):
        v = summed(g_ref, r) + bias
        v = v + jnp.where(edge, roll(at_edge[r % 5], -(32 * (r // 5) + 16)), 0.0)
        v = jnp.maximum(v, 0.0)
        if r == 0:
            v = jnp.where(s == 0, 0.0, v)
        if r == 17:
            v = jnp.where(s == NSX - 1, 0.0, v)
        em_ref[r] = v.astype(BF)
        if 1 <= r <= 16:
            cell = (r - 1) // 8
            best[cell] = v if best[cell] is None else jnp.maximum(best[cell], v)
    halves = [jnp.maximum(m, roll(m, 64)) for m in best]
    m = jnp.where(lane < 64, halves[0], halves[1])
    for shift in (-32, -16, -1, -2, -4):
        m = jnp.maximum(m, roll(m, shift))
    m = jnp.transpose(m.astype(BF).astype(F32))
    rows = [jnp.concatenate([m[64 * x : 64 * x + 1], m[64 * x + 8 : 64 * x + 9]], axis=1) for x in range(2)]
    pool_ref[...] = jnp.concatenate(rows + [jnp.zeros((6, 128), F32)], axis=0)


def k_decode(
    fl_ref, fr_ref, inner_ref, outer_ref, em_ref, we_ref, be_ref, w_ref, bias_ref, d_ref, xm, g_ref
):
    lane = lanes_of(C)
    z = jnp.bitwise_and(lane, 15)
    even = jnp.bitwise_and(lane, 16) == 0
    s, j = lax.axis_index("sx"), lax.axis_index("sy")
    blocks = []
    for g in range(5):
        hl, hr = y_halos(inner_ref, outer_ref, g)
        fl, fr = fl_ref[g], fr_ref[g]
        parts = [
            jnp.where(even, roll(fr, -16), roll(hl, 16)),
            jnp.where(even, hr, hl),
            jnp.where(even, roll(hr, -16), roll(fl, 16)),
        ]
        blocks.append(jnp.concatenate([tap for v in parts for tap in taps_of(v, z)], axis=0))
    packed = packed_products(we_ref[...], blocks)
    outside = (even & (j == NSY - 1)) | (~even & (j == 0))
    halo = []
    for g in range(5):
        v = summed_packed(packed, g) + be_ref[...]
        v = jnp.where(outside, 0.0, jnp.maximum(v, 0.0))
        if g == 0:
            v = jnp.where((lane < 32) & (s == 0), 0.0, v)
        if g == 2:
            v = jnp.where((lane >= 96) & (s == NSX - 1), 0.0, v)
        halo.append(v.astype(BF))
    for r in range(18):
        v = em_ref[r]
        beside = roll(halo[r % 5], -(32 * (r // 5) + 16))
        put_taps(
            [jnp.where(lane < 16, beside, roll(v, 16)), v, jnp.where(lane >= 112, beside, roll(v, -16))], xm, r, z
        )
    products(w_ref, xm, 0, 18, into(g_ref))
    bias = bias_ref[...]
    for x in range(16):
        d_ref[x] = summed(g_ref, x) + bias


def k_message(pair_ref, own_ref, outer_ref, out_ref):
    even = even_of("sx")
    inner, outer = jnp.where(even, pair_ref[1, 0:2], pair_ref[0, 0:2]), outer_ref[0:2]
    left, right = jnp.where(even, outer, inner), jnp.where(even, inner, outer)
    message = jnp.concatenate([left, own_ref[0:2], right, jnp.zeros((2, 128), F32)], axis=0)
    message = message.astype(BF)
    for i in range(NSY):
        out_ref[i] = message


def k_bottleneck(p_ref, vt_ref, bb_ref, ow_ref, out_ref):
    p = p_ref[...].astype(F32)
    pieces = []
    none = jnp.zeros((1, 8, 128), F32)
    for a in range(3):
        moved = p if a == 0 else jnp.concatenate([p[:, a:], p[:, :a]], axis=1)
        for b in range(3):
            if b == 0:
                v = jnp.concatenate([none, moved[:-1]], axis=0)
            elif b == 1:
                v = moved
            else:
                v = jnp.concatenate([moved[1:], none], axis=0)
            pieces.append(v.reshape(128, 128).astype(BF))
    h = dot_nt(jnp.concatenate(pieces, axis=1), vt_ref[...])
    h = jnp.maximum(h + bb_ref[...], 0.0).astype(BF)
    low = dot(h, ow_ref[...])
    zero = jnp.zeros((4, 128), F32)
    rows = [zero] + [low[8 * i : 8 * i + 4] for i in range(NSY)] + [zero, zero]
    for i in range(NSY):
        out_ref[i] = jnp.concatenate(rows[i : i + 3] + [zero], axis=0).astype(BF)


def k_final(parts_ref, s_ref, w_ref, d_ref, out_ref, xt, q_ref, buf, done, sem):
    total = parts_ref[0].astype(F32)
    for i in range(1, NSY):
        total = total + parts_ref[i].astype(F32)
    total = jnp.concatenate([total, jnp.zeros((112, 128), F32)], axis=0)
    lt = jnp.transpose(total)
    lane = lanes_of(C)
    left = []
    for cell in range(4):
        here = jnp.bitwise_and(lane, 3) == cell
        left.append(jnp.concatenate([jnp.where(here, lt[:C], 0.0), jnp.where(here, lt[C:], 0.0)], axis=1).astype(BF))
    t = dot(jnp.concatenate(left, axis=0), s_ref[...])
    for cell in range(4):
        for bc in range(9):
            xt[cell, bc, pl.ds(0, C), :] = t[C * cell : C * cell + C, 128 * bc : 128 * bc + 128].astype(BF)
    products(w_ref, xt, 0, 4, into(q_ref))
    s = lax.axis_index("sx")
    first, last = s == 0, s == NSX - 1
    copies = []
    for part in range(4):
        rows = 16
        for x in range(16):
            v = d_ref[x, pl.ds(rows * part, rows), :]
            for a in range(3):
                g = x + a - 1
                num = 2 * g - 7
                low = num // 16
                high = (num - 16 * low) / 16.0
                cell = low + 1
                w_low, w_high = jnp.float32(1.0 - high), jnp.float32(high)
                if cell == 0:
                    w_low = jnp.where(first, 0.0, w_low)
                    w_high = jnp.where(first, 0.0 if g < 0 else 1.0, w_high)
                if cell == 2:
                    w_low = jnp.where(last, 0.0 if g > 15 else 1.0, w_low)
                    w_high = jnp.where(last, 0.0, w_high)
                at = pl.ds(C * a + rows * part, rows)
                v = v + w_low * q_ref[cell, at, :]
                v = v + w_high * q_ref[cell + 1, at, :]
            buf[part, pl.ds(x, rows, stride=STRIDE), :] = v
        at = pl.ds(rows * part, rows)
        for o in range(rows):
            done[rows * part + o] = buf[part, pl.ds(STRIDE * o, 16), :].astype(BF)
        copy = pltpu.make_async_copy(done.at[at], out_ref.at[at], sem.at[part])
        copy.start()
        copies.append(copy)
    for copy in copies:
        copy.wait()


def swapped(v, axis, start):
    size = lax.axis_size(axis)
    low = range(start, size - 1, 2)
    return lax.ppermute(v, axis, [(i, i + 1) for i in low] + [(i + 1, i) for i in low])


def paired(v, axis):
    pairs = [[i, i + 1] for i in range(0, lax.axis_size(axis), 2)]
    return lax.all_gather(v, axis, axis_index_groups=pairs)


def per_device(features, enc_weight, enc_bias, proj_weight, bottle_weight, bottle_bias, out_weight, dec_weight, dec_bias):
    first = (features, enc_weight.reshape(27, C, C), enc_bias.reshape(1, C))
    deep = (bottle_weight.reshape(27 * 32, 512), proj_weight, out_weight, bottle_bias.reshape(1, 32))
    last = (dec_weight.reshape(27, C, C), dec_bias.reshape(1, C))
    ft, inner, outer, ew, eb = call(
        k_features,
        (S((18, C, 128), BF), S((2, C, 128), BF), S((2, C, 128), BF)) + tuple(S(v.shape, v.dtype) for v in first[1:]),
        *first,
        scratch=[pltpu.VMEM((C, 16, 128), BF), pltpu.VMEM((C * STRIDE, 128), F32), pltpu.SemaphoreType.DMA((3,))],
        hbm=range(3),
    )
    outer, pair = swapped(outer, "sx", 1), paired(inner, "sx")
    we, wedge, be = call(
        k_enc_weights, (S((3 * C, 9 * C), BF), S((3 * C, 6 * C), BF), S((C, 128), F32)), ew, eb, flops=10**8
    )
    xh, fl, fr, inner, outer = call(k_faces, (S((4, C, 128), BF),) + (S((5, C, 128), BF),) * 4, pair, outer, ft)
    outer, inner = swapped(outer, "sy", 1), swapped(inner, "sy", 0)
    product, *deep = call(
        k_interior,
        (S((20, 3 * C + 8, 128), F32),) + tuple(S(v.shape, v.dtype) for v in deep),
        ft,
        xh,
        we,
        *deep,
        scratch=[pltpu.VMEM((20, 9, C + 16, 128), BF), pltpu.SemaphoreType.DMA((4,))],
        flops=4 * 10**8,
        hbm=range(3, 7),
    )
    em, pooled = call(k_encode, (S((18, C, 128), BF), S((8, 128), F32)), product, inner, outer, wedge, be)
    p_outer, p_pair = swapped(pooled, "sx", 1), paired(pooled, "sx")
    vt, ow2, bb2 = call(k_weights, (S((C, 9 * 128), BF), S((C, 128), BF), S((1, C), F32)), *deep, flops=4 * 10**8)
    wd, bd, smat = call(
        k_dec_weights,
        (S((3 * C, 9 * C), BF), S((C, 128), F32), S((256, 9 * 128), BF)),
        *last,
        scratch=[pltpu.VMEM(v.shape, v.dtype) for v in last] + [pltpu.SemaphoreType.DMA((2,))],
        flops=10**8,
        hbm=(0, 1),
    )
    d = call(
        k_decode,
        S((16, C, 128), F32),
        fl,
        fr,
        inner,
        outer,
        em,
        we,
        be,
        wd,
        bd,
        scratch=[pltpu.VMEM((18, 9, C + 16, 128), BF), pltpu.VMEM((18, 3 * C + 8, 128), F32)],
        flops=4 * 10**8,
    )
    message = call(k_message, S((NSY, 8, 128), BF), p_pair, pooled, p_outer)
    everyone = lax.all_to_all(message, "sy", 0, 0, tiled=True)
    partial = call(k_bottleneck, S((NSY, 16, 128), BF), everyone, vt, bb2, ow2)
    parts = lax.all_to_all(partial, "sy", 0, 0, tiled=True)
    return call(
        k_final,
        S((C, 16, 128), BF),
        parts,
        smat,
        wd,
        d,
        scratch=[
            pltpu.VMEM((4, 9, C + 16, 128), BF),
            pltpu.VMEM((4, 3 * C + 8, 128), F32),
            pltpu.VMEM((4, 16 * STRIDE, 128), F32),
            pltpu.VMEM((C, 16, 128), BF),
            pltpu.SemaphoreType.DMA((4,)),
        ],
        out_space=pltpu.HBM,
    )


def solution(mesh):
    in_specs = (P(None, "sx", "sy"), P(), P(), P(), P(None, None, None, "sy", None), P("sy"), P("sy", None), P(), P())

    return jax.shard_map(per_device, mesh=mesh, in_specs=in_specs, out_specs=P(None, "sx", "sy"), check_vma=False)
```

```python
import jax
import jax.numpy as jnp
from jax import lax
from jax.experimental import pallas as pl
from jax.experimental.pallas import tpu as pltpu
from jax.sharding import PartitionSpec as P


F32 = jnp.float32
BF = jnp.bfloat16
C = 64
NSX = 32
NSY = 16
STRIDE = 17


def call(kernel, outs, *ins, scratch=(), flops=1000000, limit=16, hbm=(), out_space=pltpu.VMEM):
    ins = [pltpu.with_memory_space_constraint(v, pltpu.HBM) if i in hbm else v for i, v in enumerate(ins)]
    return pl.pallas_call(
        kernel,
        out_shape=outs,
        in_specs=[pl.BlockSpec(memory_space=pltpu.HBM if i in hbm else pltpu.VMEM) for i in range(len(ins))],
        out_specs=jax.tree.map(lambda _: pl.BlockSpec(memory_space=out_space), outs),
        scratch_shapes=list(scratch),
        compiler_params=pltpu.CompilerParams(vmem_limit_bytes=limit * 2**20),
        cost_estimate=pl.CostEstimate(flops=flops, transcendentals=0, bytes_accessed=100000),
    )(*ins)


def S(shape, dtype):
    return jax.ShapeDtypeStruct(shape, dtype)


def dot(a, b):
    return jnp.dot(a, b, preferred_element_type=F32)


def dot_nt(a, b):
    return lax.dot_general(a, b, (((1,), (1,)), ((), ())), preferred_element_type=F32)


def lanes_of(rows):
    return lax.broadcasted_iota(jnp.int32, (rows, 128), 1)


def roll(v, shift):
    shift = shift % 128
    return v if shift == 0 else pltpu.roll(v, shift, 1)


def even_of(axis):
    return lax.rem(lax.axis_index(axis), 2) == 0


def fetches(sources, targets, sem):
    copies = [pltpu.make_async_copy(a, b, sem.at[i]) for i, (a, b) in enumerate(zip(sources, targets))]
    for copy in copies:
        copy.start()
    return copies


def k_features(x_ref, ew_hbm, eb_hbm, ft_ref, inner_ref, outer_ref, ew_ref, eb_ref, held, buf, sem):
    copies = fetches((x_ref, ew_hbm, eb_hbm), (held, ew_ref, eb_ref), sem)
    even = even_of("sx")
    copies[0].wait()
    for c in range(C):
        buf[pl.ds(STRIDE * c, 16), :] = held[c].astype(F32)

    def row(x):
        return buf[pl.ds(x, C, stride=STRIDE), :]

    for k in range(2):
        low, high = row(k), row(14 + k)
        inner_ref[k] = jnp.where(even, high, low).astype(BF)
        outer_ref[k] = jnp.where(even, low, high).astype(BF)
    for x in range(16):
        ft_ref[x + 2] = row(x).astype(BF)
    for copy in copies[1:]:
        copy.wait()


def k_faces(pair_ref, outer_ref, ft_ref, x_ref, left_ref, right_ref, s_inner_ref, s_outer_ref):
    lane = lanes_of(C)
    even_x, even_y = even_of("sx"), even_of("sy")
    for k in range(2):
        inner, outer = jnp.where(even_x, pair_ref[1, k], pair_ref[0, k]), outer_ref[k]
        x_ref[k] = jnp.where(even_x, outer, inner)
        x_ref[2 + k] = jnp.where(even_x, inner, outer)
    for g in range(5):
        left = None
        for q in range(4):
            r = 5 * q + g
            v = x_ref[r] if r < 2 else ft_ref[r] if r < 18 else x_ref[r - 16]
            v = v.astype(F32)
            a, b = roll(v, 32 * q), roll(v, 32 * q - 96)
            if q == 0:
                left, right = a, b
            else:
                here = lane >= 32 * q
                left, right = jnp.where(here, a, left), jnp.where(here, b, right)
        left_ref[g] = left.astype(BF)
        right_ref[g] = right.astype(BF)
        s_inner_ref[g] = jnp.where(even_y, right, left).astype(BF)
        s_outer_ref[g] = jnp.where(even_y, left, right).astype(BF)


def arranged(w_ref, out_ref, taps):
    for a in range(3):
        for at in range(0, len(taps), 2):
            blocks = [w_ref[a * 9 + t] for t in taps[at : at + 2]]
            wide = blocks[0] if len(blocks) == 1 else jnp.concatenate(blocks, axis=1)
            out_ref[pl.ds(a * C, C), pl.ds(C * at, wide.shape[1])] = wide


def column(b_ref):
    row = jnp.broadcast_to(b_ref[...], (C, C))
    same = lax.broadcasted_iota(jnp.int32, (C, C), 0) == lax.broadcasted_iota(jnp.int32, (C, C), 1)
    return jnp.broadcast_to(jnp.sum(jnp.where(same, row, 0.0), axis=1, keepdims=True), (C, 128))


def interp_weight(g, cell, count, cells):
    num = 2 * g - 7
    low = jnp.right_shift(num, 4)
    w = (num - 16 * low).astype(F32) * (1.0 / 16.0)
    w = jnp.where((low < 0) | (low >= cells - 1), 0.0, w)
    low = jnp.clip(low, 0, cells - 1)
    value = jnp.where(cell == low, 1.0 - w, jnp.where(cell == low + 1, w, 0.0))
    return jnp.where((g >= 0) & (g < count), value, 0.0)


def k_enc_weights(ew, eb, we_ref, wedge_ref, be_ref):
    arranged(ew, we_ref, range(9))
    arranged(ew, wedge_ref, (0, 1, 2, 6, 7, 8))
    be_ref[...] = column(eb)


def k_weights(bw, proj, ow, bb, vt_ref, ow2_ref, bb2_ref):
    p = proj[...]
    r = dot_nt(bw[...], jnp.concatenate([p, p], axis=0))
    half = lanes_of(C) < C
    for ab in range(9):
        both = jnp.where(half, r[96 * ab : 96 * ab + 64], r[96 * ab + 32 : 96 * ab + 96])
        vt_ref[:, pl.ds(128 * ab, 128)] = both.astype(BF)
    o = ow[...]
    none = jnp.zeros_like(o)
    ow2_ref[...] = jnp.concatenate([jnp.concatenate([o, none], axis=1), jnp.concatenate([none, o], axis=1)], axis=0)
    bb2_ref[...] = jnp.concatenate([bb[...], bb[...]], axis=1)


def k_dec_weights(dw_hbm, db_hbm, wd_ref, bd_ref, s_ref, dw, db, sem):
    copies = fetches((dw_hbm, db_hbm), (dw, db), sem)
    j = lax.axis_index("sy")
    row = lax.broadcasted_iota(jnp.int32, (16, 128), 0)
    lane = lax.broadcasted_iota(jnp.int32, (16, 128), 1)
    y, z = jnp.right_shift(lane, 4), jnp.bitwise_and(lane, 15)
    cell_y = j - 1 + jnp.right_shift(row, 2)
    zero = jnp.zeros((112, 128), BF)
    for b in range(3):
        wy = interp_weight(8 * j + y + (b - 1), cell_y, 8 * NSY, NSY)
        wy = jnp.where(row < 12, wy, 0.0)
        for c in range(3):
            for zo in range(2):
                wz = interp_weight(z + (c - 1), 1 - zo, 16, 2)
                at = pl.ds(128 * (3 * b + c), 128)
                s_ref[pl.ds(128 * zo, 16), at] = (wy * wz).astype(BF)
                s_ref[pl.ds(128 * zo + 16, 112), at] = zero
    for copy in copies:
        copy.wait()
    arranged(dw, wd_ref, range(9))
    bd_ref[...] = column(db)


def taps_of(v, z):
    zero = jnp.zeros_like(v)
    return [jnp.where(z == 0, zero, roll(v, 1)), v, jnp.where(z == 15, zero, roll(v, -1))]


def put_taps(parts, xm, n, z):
    for b, v in enumerate(parts):
        for c, tap in enumerate(taps_of(v, z)):
            xm[n, 3 * b + c, pl.ds(0, C), :] = tap


def products(w_ref, xm, first, last, store):
    w = w_ref[...]

    def block(n):
        return jnp.concatenate([xm[n, t, pl.ds(0, C), :] for t in range(9)], axis=0)

    for n in range(first, last, 2):
        if n + 1 < last:
            g = dot(w, jnp.concatenate([block(n), block(n + 1)], axis=1))
            store(n, g[:, :128])
            store(n + 1, g[:, 128:])
        else:
            store(n, dot(w, block(n)))


def into(g_ref):
    def store(n, g):
        g_ref[n, pl.ds(0, 3 * C), :] = g

    return store


def summed(g_ref, r):
    return g_ref[r, pl.ds(0, C), :] + g_ref[r + 1, pl.ds(C, C), :] + g_ref[r + 2, pl.ds(2 * C, C), :]


def summed_packed(packed, g):
    v = packed[g][:C]
    for a in (1, 2):
        tap = packed[(g + a) % 5][a * C : a * C + C]
        v = v + (tap if g + a < 5 else roll(tap, -32))
    return v


def packed_products(w, blocks):
    out = []
    for n in range(0, 5, 2):
        if n + 1 < 5:
            g = dot(w, jnp.concatenate([blocks[n], blocks[n + 1]], axis=1))
            out += [g[:, :128], g[:, 128:]]
        else:
            out.append(dot(w, blocks[n]))
    return out


def y_halos(inner_ref, outer_ref, g):
    even_y = even_of("sy")
    inner, outer = inner_ref[g], outer_ref[g]
    return jnp.where(even_y, outer, inner), jnp.where(even_y, inner, outer)


def k_interior(ft_ref, x_ref, w_ref, *refs):
    sources, g_ref, targets, xm, sem = refs[:3], refs[3], refs[4:7], refs[7], refs[8]
    copies = fetches(sources, targets, sem)
    lane = lanes_of(C)
    z = jnp.bitwise_and(lane, 15)
    for r in range(20):
        v = x_ref[r] if r < 2 else ft_ref[r] if r < 18 else x_ref[r - 16]
        zero = jnp.zeros_like(v)
        put_taps(
            [jnp.where(lane < 16, zero, roll(v, 16)), v, jnp.where(lane >= 112, zero, roll(v, -16))], xm, r, z
        )
    products(w_ref, xm, 0, 20, into(g_ref))
    for copy in copies:
        copy.wait()


def k_encode(g_ref, inner_ref, outer_ref, w_ref, bias_ref, em_ref, pool_ref):
    lane = lanes_of(C)
    z = jnp.bitwise_and(lane, 15)
    even = jnp.bitwise_and(lane, 16) == 0
    edge = (lane < 16) | (lane >= 112)
    s = lax.axis_index("sx")
    blocks = []
    for g in range(5):
        hl, hr = y_halos(inner_ref, outer_ref, g)
        zero = jnp.zeros_like(hl)
        low, high = jnp.where(even, zero, hl), jnp.where(even, hr, zero)
        blocks.append(jnp.concatenate(taps_of(low, z) + taps_of(high, z), axis=0))
    packed = packed_products(w_ref[...], blocks)
    bias = bias_ref[...]
    best = [None, None]
    at_edge = [summed_packed(packed, g) for g in range(5)]
    for r in range(18):
        v = summed(g_ref, r) + bias
        v = v + jnp.where(edge, roll(at_edge[r % 5], -(32 * (r // 5) + 16)), 0.0)
        v = jnp.maximum(v, 0.0)
        if r == 0:
            v = jnp.where(s == 0, 0.0, v)
        if r == 17:
            v = jnp.where(s == NSX - 1, 0.0, v)
        em_ref[r] = v.astype(BF)
        if 1 <= r <= 16:
            cell = (r - 1) // 8
            best[cell] = v if best[cell] is None else jnp.maximum(best[cell], v)
    halves = [jnp.maximum(m, roll(m, 64)) for m in best]
    m = jnp.where(lane < 64, halves[0], halves[1])
    for shift in (-32, -16, -1, -2, -4):
        m = jnp.maximum(m, roll(m, shift))
    m = jnp.transpose(m.astype(BF).astype(F32))
    rows = [jnp.concatenate([m[64 * x : 64 * x + 1], m[64 * x + 8 : 64 * x + 9]], axis=1) for x in range(2)]
    pool_ref[...] = jnp.concatenate(rows + [jnp.zeros((6, 128), F32)], axis=0)


def k_decode(
    fl_ref, fr_ref, inner_ref, outer_ref, em_ref, we_ref, be_ref, w_ref, bias_ref, d_ref, xm, g_ref
):
    lane = lanes_of(C)
    z = jnp.bitwise_and(lane, 15)
    even = jnp.bitwise_and(lane, 16) == 0
    s, j = lax.axis_index("sx"), lax.axis_index("sy")
    blocks = []
    for g in range(5):
        hl, hr = y_halos(inner_ref, outer_ref, g)
        fl, fr = fl_ref[g], fr_ref[g]
        parts = [
            jnp.where(even, roll(fr, -16), roll(hl, 16)),
            jnp.where(even, hr, hl),
            jnp.where(even, roll(hr, -16), roll(fl, 16)),
        ]
        blocks.append(jnp.concatenate([tap for v in parts for tap in taps_of(v, z)], axis=0))
    packed = packed_products(we_ref[...], blocks)
    outside = (even & (j == NSY - 1)) | (~even & (j == 0))
    halo = []
    for g in range(5):
        v = summed_packed(packed, g) + be_ref[...]
        v = jnp.where(outside, 0.0, jnp.maximum(v, 0.0))
        if g == 0:
            v = jnp.where((lane < 32) & (s == 0), 0.0, v)
        if g == 2:
            v = jnp.where((lane >= 96) & (s == NSX - 1), 0.0, v)
        halo.append(v.astype(BF))
    for r in range(18):
        v = em_ref[r]
        beside = roll(halo[r % 5], -(32 * (r // 5) + 16))
        put_taps(
            [jnp.where(lane < 16, beside, roll(v, 16)), v, jnp.where(lane >= 112, beside, roll(v, -16))], xm, r, z
        )
    products(w_ref, xm, 0, 18, into(g_ref))
    bias = bias_ref[...]
    for x in range(16):
        d_ref[x] = summed(g_ref, x) + bias


def k_message(pair_ref, own_ref, outer_ref, out_ref):
    even = even_of("sx")
    inner, outer = jnp.where(even, pair_ref[1, 0:2], pair_ref[0, 0:2]), outer_ref[0:2]
    left, right = jnp.where(even, outer, inner), jnp.where(even, inner, outer)
    message = jnp.concatenate([left, own_ref[0:2], right, jnp.zeros((2, 128), F32)], axis=0)
    message = message.astype(BF)
    for i in range(NSY):
        out_ref[i] = message


def k_bottleneck(p_ref, vt_ref, bb_ref, ow_ref, out_ref):
    p = p_ref[...].astype(F32)
    pieces = []
    none = jnp.zeros((1, 8, 128), F32)
    for a in range(3):
        moved = p if a == 0 else jnp.concatenate([p[:, a:], p[:, :a]], axis=1)
        for b in range(3):
            if b == 0:
                v = jnp.concatenate([none, moved[:-1]], axis=0)
            elif b == 1:
                v = moved
            else:
                v = jnp.concatenate([moved[1:], none], axis=0)
            pieces.append(v.reshape(128, 128).astype(BF))
    h = dot_nt(jnp.concatenate(pieces, axis=1), vt_ref[...])
    h = jnp.maximum(h + bb_ref[...], 0.0).astype(BF)
    low = dot(h, ow_ref[...])
    zero = jnp.zeros((4, 128), F32)
    rows = [zero] + [low[8 * i : 8 * i + 4] for i in range(NSY)] + [zero, zero]
    for i in range(NSY):
        out_ref[i] = jnp.concatenate(rows[i : i + 3] + [zero], axis=0).astype(BF)


def k_final(parts_ref, s_ref, w_ref, d_ref, out_ref, xt, q_ref, buf, done, sem):
    total = parts_ref[0].astype(F32)
    for i in range(1, NSY):
        total = total + parts_ref[i].astype(F32)
    total = jnp.concatenate([total, jnp.zeros((112, 128), F32)], axis=0)
    lt = jnp.transpose(total)
    lane = lanes_of(C)
    left = []
    for cell in range(4):
        here = jnp.bitwise_and(lane, 3) == cell
        left.append(jnp.concatenate([jnp.where(here, lt[:C], 0.0), jnp.where(here, lt[C:], 0.0)], axis=1).astype(BF))
    t = dot(jnp.concatenate(left, axis=0), s_ref[...])
    for cell in range(4):
        for bc in range(9):
            xt[cell, bc, pl.ds(0, C), :] = t[C * cell : C * cell + C, 128 * bc : 128 * bc + 128].astype(BF)
    products(w_ref, xt, 0, 4, into(q_ref))
    s = lax.axis_index("sx")
    first, last = s == 0, s == NSX - 1
    copies = []
    for part in range(4):
        rows = 16
        for x in range(16):
            v = d_ref[x, pl.ds(rows * part, rows), :]
            for a in range(3):
                g = x + a - 1
                num = 2 * g - 7
                low = num // 16
                high = (num - 16 * low) / 16.0
                cell = low + 1
                w_low, w_high = jnp.float32(1.0 - high), jnp.float32(high)
                if cell == 0:
                    w_low = jnp.where(first, 0.0, w_low)
                    w_high = jnp.where(first, 0.0 if g < 0 else 1.0, w_high)
                if cell == 2:
                    w_low = jnp.where(last, 0.0 if g > 15 else 1.0, w_low)
                    w_high = jnp.where(last, 0.0, w_high)
                at = pl.ds(C * a + rows * part, rows)
                v = v + w_low * q_ref[cell, at, :]
                v = v + w_high * q_ref[cell + 1, at, :]
            buf[part, pl.ds(x, rows, stride=STRIDE), :] = v
        at = pl.ds(rows * part, rows)
        for o in range(rows):
            done[rows * part + o] = buf[part, pl.ds(STRIDE * o, 16), :].astype(BF)
        copy = pltpu.make_async_copy(done.at[at], out_ref.at[at], sem.at[part])
        copy.start()
        copies.append(copy)
    for copy in copies:
        copy.wait()


def swapped(v, axis, start):
    size = lax.axis_size(axis)
    low = range(start, size - 1, 2)
    return lax.ppermute(v, axis, [(i, i + 1) for i in low] + [(i + 1, i) for i in low])


def paired(v, axis):
    pairs = [[i, i + 1] for i in range(0, lax.axis_size(axis), 2)]
    return lax.all_gather(v, axis, axis_index_groups=pairs)


def per_device(features, enc_weight, enc_bias, proj_weight, bottle_weight, bottle_bias, out_weight, dec_weight, dec_bias):
    first = (features, enc_weight.reshape(27, C, C), enc_bias.reshape(1, C))
    deep = (proj_weight, out_weight, bottle_bias.reshape(1, 32))
    last = (dec_weight.reshape(27, C, C), dec_bias.reshape(1, C))
    ft, inner, outer, ew, eb = call(
        k_features,
        (S((18, C, 128), BF), S((2, C, 128), BF), S((2, C, 128), BF)) + tuple(S(v.shape, v.dtype) for v in first[1:]),
        *first,
        scratch=[pltpu.VMEM((C, 16, 128), BF), pltpu.VMEM((C * STRIDE, 128), F32), pltpu.SemaphoreType.DMA((3,))],
        hbm=range(3),
    )
    outer, pair = swapped(outer, "sx", 1), paired(inner, "sx")
    we, wedge, be = call(
        k_enc_weights, (S((3 * C, 9 * C), BF), S((3 * C, 6 * C), BF), S((C, 128), F32)), ew, eb, flops=10**8
    )
    xh, fl, fr, inner, outer = call(k_faces, (S((4, C, 128), BF),) + (S((5, C, 128), BF),) * 4, pair, outer, ft)
    outer, inner = swapped(outer, "sy", 1), swapped(inner, "sy", 0)
    product, *deep = call(
        k_interior,
        (S((20, 3 * C + 8, 128), F32),) + tuple(S(v.shape, v.dtype) for v in deep),
        ft,
        xh,
        we,
        *deep,
        scratch=[pltpu.VMEM((20, 9, C + 16, 128), BF), pltpu.SemaphoreType.DMA((3,))],
        flops=4 * 10**8,
        hbm=range(3, 6),
    )
    em, pooled = call(k_encode, (S((18, C, 128), BF), S((8, 128), F32)), product, inner, outer, wedge, be)
    p_outer, p_pair = swapped(pooled, "sx", 1), paired(pooled, "sx")
    vt, ow2, bb2 = call(
        k_weights,
        (S((C, 9 * 128), BF), S((C, 128), BF), S((1, C), F32)),
        bottle_weight.reshape(27 * 32, 512),
        *deep,
        flops=4 * 10**8,
    )
    wd, bd, smat = call(
        k_dec_weights,
        (S((3 * C, 9 * C), BF), S((C, 128), F32), S((256, 9 * 128), BF)),
        *last,
        scratch=[pltpu.VMEM(v.shape, v.dtype) for v in last] + [pltpu.SemaphoreType.DMA((2,))],
        flops=10**8,
        hbm=(0, 1),
    )
    d = call(
        k_decode,
        S((16, C, 128), F32),
        fl,
        fr,
        inner,
        outer,
        em,
        we,
        be,
        wd,
        bd,
        scratch=[pltpu.VMEM((18, 9, C + 16, 128), BF), pltpu.VMEM((18, 3 * C + 8, 128), F32)],
        flops=4 * 10**8,
    )
    message = call(k_message, S((NSY, 8, 128), BF), p_pair, pooled, p_outer)
    everyone = lax.all_to_all(message, "sy", 0, 0, tiled=True)
    partial = call(k_bottleneck, S((NSY, 16, 128), BF), everyone, vt, bb2, ow2)
    parts = lax.all_to_all(partial, "sy", 0, 0, tiled=True)
    return call(
        k_final,
        S((C, 16, 128), BF),
        parts,
        smat,
        wd,
        d,
        scratch=[
            pltpu.VMEM((4, 9, C + 16, 128), BF),
            pltpu.VMEM((4, 3 * C + 8, 128), F32),
            pltpu.VMEM((4, 16 * STRIDE, 128), F32),
            pltpu.VMEM((C, 16, 128), BF),
            pltpu.SemaphoreType.DMA((4,)),
        ],
        out_space=pltpu.HBM,
    )


def solution(mesh):
    in_specs = (P(None, "sx", "sy"), P(), P(), P(), P(None, None, None, "sy", None), P("sy"), P("sy", None), P(), P())

    return jax.shard_map(per_device, mesh=mesh, in_specs=in_specs, out_specs=P(None, "sx", "sy"), check_vma=False)
```

```python
import jax
import jax.numpy as jnp
from jax import lax
from jax.experimental import pallas as pl
from jax.experimental.pallas import tpu as pltpu
from jax.sharding import PartitionSpec as P


F32 = jnp.float32
BF = jnp.bfloat16
C = 64
NSX = 32
NSY = 16
STRIDE = 17


def call(kernel, outs, *ins, scratch=(), flops=1000000, limit=16, hbm=(), out_space=pltpu.VMEM):
    ins = [pltpu.with_memory_space_constraint(v, pltpu.HBM) if i in hbm else v for i, v in enumerate(ins)]
    return pl.pallas_call(
        kernel,
        out_shape=outs,
        in_specs=[pl.BlockSpec(memory_space=pltpu.HBM if i in hbm else pltpu.VMEM) for i in range(len(ins))],
        out_specs=jax.tree.map(lambda _: pl.BlockSpec(memory_space=out_space), outs),
        scratch_shapes=list(scratch),
        compiler_params=pltpu.CompilerParams(vmem_limit_bytes=limit * 2**20),
        cost_estimate=pl.CostEstimate(flops=flops, transcendentals=0, bytes_accessed=100000),
    )(*ins)


def S(shape, dtype):
    return jax.ShapeDtypeStruct(shape, dtype)


def dot(a, b):
    return jnp.dot(a, b, preferred_element_type=F32)


def dot_nt(a, b):
    return lax.dot_general(a, b, (((1,), (1,)), ((), ())), preferred_element_type=F32)


def lanes_of(rows):
    return lax.broadcasted_iota(jnp.int32, (rows, 128), 1)


def roll(v, shift):
    shift = shift % 128
    return v if shift == 0 else pltpu.roll(v, shift, 1)


def even_of(axis):
    return lax.rem(lax.axis_index(axis), 2) == 0


def fetches(sources, targets, sem):
    copies = [pltpu.make_async_copy(a, b, sem.at[i]) for i, (a, b) in enumerate(zip(sources, targets))]
    for copy in copies:
        copy.start()
    return copies


def k_features(*refs):
    x_ref, sources, (ft_ref, inner_ref, outer_ref), targets = refs[0], refs[1:6], refs[6:9], refs[9:14]
    held, buf, sem = refs[14:]
    copies = fetches((x_ref, *sources), (held, *targets), sem)
    even = even_of("sx")
    copies[0].wait()
    for c in range(C):
        buf[pl.ds(STRIDE * c, 16), :] = held[c].astype(F32)

    def row(x):
        return buf[pl.ds(x, C, stride=STRIDE), :]

    for k in range(2):
        low, high = row(k), row(14 + k)
        inner_ref[k] = jnp.where(even, high, low).astype(BF)
        outer_ref[k] = jnp.where(even, low, high).astype(BF)
    for x in range(16):
        ft_ref[x + 2] = row(x).astype(BF)
    for copy in copies[1:]:
        copy.wait()


def k_faces(pair_ref, outer_ref, ft_ref, x_ref, left_ref, right_ref, s_inner_ref, s_outer_ref):
    lane = lanes_of(C)
    even_x, even_y = even_of("sx"), even_of("sy")
    for k in range(2):
        inner, outer = jnp.where(even_x, pair_ref[1, k], pair_ref[0, k]), outer_ref[k]
        x_ref[k] = jnp.where(even_x, outer, inner)
        x_ref[2 + k] = jnp.where(even_x, inner, outer)
    for g in range(5):
        left = None
        for q in range(4):
            r = 5 * q + g
            v = x_ref[r] if r < 2 else ft_ref[r] if r < 18 else x_ref[r - 16]
            v = v.astype(F32)
            a, b = roll(v, 32 * q), roll(v, 32 * q - 96)
            if q == 0:
                left, right = a, b
            else:
                here = lane >= 32 * q
                left, right = jnp.where(here, a, left), jnp.where(here, b, right)
        left_ref[g] = left.astype(BF)
        right_ref[g] = right.astype(BF)
        s_inner_ref[g] = jnp.where(even_y, right, left).astype(BF)
        s_outer_ref[g] = jnp.where(even_y, left, right).astype(BF)


def arranged(w_ref, out_ref, taps):
    for a in range(3):
        for at in range(0, len(taps), 2):
            blocks = [w_ref[a * 9 + t] for t in taps[at : at + 2]]
            wide = blocks[0] if len(blocks) == 1 else jnp.concatenate(blocks, axis=1)
            out_ref[pl.ds(a * C, C), pl.ds(C * at, wide.shape[1])] = wide


def column(b_ref):
    row = jnp.broadcast_to(b_ref[...], (C, C))
    same = lax.broadcasted_iota(jnp.int32, (C, C), 0) == lax.broadcasted_iota(jnp.int32, (C, C), 1)
    return jnp.broadcast_to(jnp.sum(jnp.where(same, row, 0.0), axis=1, keepdims=True), (C, 128))


def interp_weight(g, cell, count, cells):
    num = 2 * g - 7
    low = jnp.right_shift(num, 4)
    w = (num - 16 * low).astype(F32) * (1.0 / 16.0)
    w = jnp.where((low < 0) | (low >= cells - 1), 0.0, w)
    low = jnp.clip(low, 0, cells - 1)
    value = jnp.where(cell == low, 1.0 - w, jnp.where(cell == low + 1, w, 0.0))
    return jnp.where((g >= 0) & (g < count), value, 0.0)


def k_enc_weights(ew, eb, we_ref, wedge_ref, be_ref):
    arranged(ew, we_ref, range(9))
    arranged(ew, wedge_ref, (0, 1, 2, 6, 7, 8))
    be_ref[...] = column(eb)


def k_weights(bw, proj, ow, bb, vt_ref, ow2_ref, bb2_ref):
    p = proj[...]
    r = dot_nt(bw[...], jnp.concatenate([p, p], axis=0))
    half = lanes_of(C) < C
    for ab in range(9):
        both = jnp.where(half, r[96 * ab : 96 * ab + 64], r[96 * ab + 32 : 96 * ab + 96])
        vt_ref[:, pl.ds(128 * ab, 128)] = both.astype(BF)
    o = ow[...]
    none = jnp.zeros_like(o)
    ow2_ref[...] = jnp.concatenate([jnp.concatenate([o, none], axis=1), jnp.concatenate([none, o], axis=1)], axis=0)
    bb2_ref[...] = jnp.concatenate([bb[...], bb[...]], axis=1)


def k_dec_weights(dw_hbm, db_hbm, wd_ref, bd_ref, s_ref, dw, db, sem):
    copies = fetches((dw_hbm, db_hbm), (dw, db), sem)
    j = lax.axis_index("sy")
    row = lax.broadcasted_iota(jnp.int32, (16, 128), 0)
    lane = lax.broadcasted_iota(jnp.int32, (16, 128), 1)
    y, z = jnp.right_shift(lane, 4), jnp.bitwise_and(lane, 15)
    cell_y = j - 1 + jnp.right_shift(row, 2)
    zero = jnp.zeros((112, 128), BF)
    for b in range(3):
        wy = interp_weight(8 * j + y + (b - 1), cell_y, 8 * NSY, NSY)
        wy = jnp.where(row < 12, wy, 0.0)
        for c in range(3):
            for zo in range(2):
                wz = interp_weight(z + (c - 1), 1 - zo, 16, 2)
                at = pl.ds(128 * (3 * b + c), 128)
                s_ref[pl.ds(128 * zo, 16), at] = (wy * wz).astype(BF)
                s_ref[pl.ds(128 * zo + 16, 112), at] = zero
    for copy in copies:
        copy.wait()
    arranged(dw, wd_ref, range(9))
    bd_ref[...] = column(db)


def taps_of(v, z):
    zero = jnp.zeros_like(v)
    return [jnp.where(z == 0, zero, roll(v, 1)), v, jnp.where(z == 15, zero, roll(v, -1))]


def put_taps(parts, xm, n, z):
    for b, v in enumerate(parts):
        for c, tap in enumerate(taps_of(v, z)):
            xm[n, 3 * b + c, pl.ds(0, C), :] = tap


def products(w_ref, xm, first, last, store):
    w = w_ref[...]

    def block(n):
        return jnp.concatenate([xm[n, t, pl.ds(0, C), :] for t in range(9)], axis=0)

    for n in range(first, last, 2):
        if n + 1 < last:
            g = dot(w, jnp.concatenate([block(n), block(n + 1)], axis=1))
            store(n, g[:, :128])
            store(n + 1, g[:, 128:])
        else:
            store(n, dot(w, block(n)))


def into(g_ref):
    def store(n, g):
        g_ref[n, pl.ds(0, 3 * C), :] = g

    return store


def summed(g_ref, r):
    return g_ref[r, pl.ds(0, C), :] + g_ref[r + 1, pl.ds(C, C), :] + g_ref[r + 2, pl.ds(2 * C, C), :]


def summed_packed(packed, g):
    v = packed[g][:C]
    for a in (1, 2):
        tap = packed[(g + a) % 5][a * C : a * C + C]
        v = v + (tap if g + a < 5 else roll(tap, -32))
    return v


def packed_products(w, blocks):
    out = []
    for n in range(0, 5, 2):
        if n + 1 < 5:
            g = dot(w, jnp.concatenate([blocks[n], blocks[n + 1]], axis=1))
            out += [g[:, :128], g[:, 128:]]
        else:
            out.append(dot(w, blocks[n]))
    return out


def y_halos(inner_ref, outer_ref, g):
    even_y = even_of("sy")
    inner, outer = inner_ref[g], outer_ref[g]
    return jnp.where(even_y, outer, inner), jnp.where(even_y, inner, outer)


def k_interior(ft_ref, x_ref, w_ref, g_ref, xm):
    lane = lanes_of(C)
    z = jnp.bitwise_and(lane, 15)
    for r in range(20):
        v = x_ref[r] if r < 2 else ft_ref[r] if r < 18 else x_ref[r - 16]
        zero = jnp.zeros_like(v)
        put_taps(
            [jnp.where(lane < 16, zero, roll(v, 16)), v, jnp.where(lane >= 112, zero, roll(v, -16))], xm, r, z
        )
    products(w_ref, xm, 0, 20, into(g_ref))


def k_encode(g_ref, inner_ref, outer_ref, w_ref, bias_ref, em_ref, pool_ref):
    lane = lanes_of(C)
    z = jnp.bitwise_and(lane, 15)
    even = jnp.bitwise_and(lane, 16) == 0
    edge = (lane < 16) | (lane >= 112)
    s = lax.axis_index("sx")
    blocks = []
    for g in range(5):
        hl, hr = y_halos(inner_ref, outer_ref, g)
        zero = jnp.zeros_like(hl)
        low, high = jnp.where(even, zero, hl), jnp.where(even, hr, zero)
        blocks.append(jnp.concatenate(taps_of(low, z) + taps_of(high, z), axis=0))
    packed = packed_products(w_ref[...], blocks)
    bias = bias_ref[...]
    best = [None, None]
    at_edge = [summed_packed(packed, g) for g in range(5)]
    for r in range(18):
        v = summed(g_ref, r) + bias
        v = v + jnp.where(edge, roll(at_edge[r % 5], -(32 * (r // 5) + 16)), 0.0)
        v = jnp.maximum(v, 0.0)
        if r == 0:
            v = jnp.where(s == 0, 0.0, v)
        if r == 17:
            v = jnp.where(s == NSX - 1, 0.0, v)
        em_ref[r] = v.astype(BF)
        if 1 <= r <= 16:
            cell = (r - 1) // 8
            best[cell] = v if best[cell] is None else jnp.maximum(best[cell], v)
    halves = [jnp.maximum(m, roll(m, 64)) for m in best]
    m = jnp.where(lane < 64, halves[0], halves[1])
    for shift in (-32, -16, -1, -2, -4):
        m = jnp.maximum(m, roll(m, shift))
    m = jnp.transpose(m.astype(BF).astype(F32))
    rows = [jnp.concatenate([m[64 * x : 64 * x + 1], m[64 * x + 8 : 64 * x + 9]], axis=1) for x in range(2)]
    pool_ref[...] = jnp.concatenate(rows + [jnp.zeros((6, 128), F32)], axis=0)


def k_decode(
    fl_ref, fr_ref, inner_ref, outer_ref, em_ref, we_ref, be_ref, w_ref, bias_ref, d_ref, xm, g_ref
):
    lane = lanes_of(C)
    z = jnp.bitwise_and(lane, 15)
    even = jnp.bitwise_and(lane, 16) == 0
    s, j = lax.axis_index("sx"), lax.axis_index("sy")
    blocks = []
    for g in range(5):
        hl, hr = y_halos(inner_ref, outer_ref, g)
        fl, fr = fl_ref[g], fr_ref[g]
        parts = [
            jnp.where(even, roll(fr, -16), roll(hl, 16)),
            jnp.where(even, hr, hl),
            jnp.where(even, roll(hr, -16), roll(fl, 16)),
        ]
        blocks.append(jnp.concatenate([tap for v in parts for tap in taps_of(v, z)], axis=0))
    packed = packed_products(we_ref[...], blocks)
    outside = (even & (j == NSY - 1)) | (~even & (j == 0))
    halo = []
    for g in range(5):
        v = summed_packed(packed, g) + be_ref[...]
        v = jnp.where(outside, 0.0, jnp.maximum(v, 0.0))
        if g == 0:
            v = jnp.where((lane < 32) & (s == 0), 0.0, v)
        if g == 2:
            v = jnp.where((lane >= 96) & (s == NSX - 1), 0.0, v)
        halo.append(v.astype(BF))
    for r in range(18):
        v = em_ref[r]
        beside = roll(halo[r % 5], -(32 * (r // 5) + 16))
        put_taps(
            [jnp.where(lane < 16, beside, roll(v, 16)), v, jnp.where(lane >= 112, beside, roll(v, -16))], xm, r, z
        )
    products(w_ref, xm, 0, 18, into(g_ref))
    bias = bias_ref[...]
    for x in range(16):
        d_ref[x] = summed(g_ref, x) + bias


def k_message(pair_ref, own_ref, outer_ref, out_ref):
    even = even_of("sx")
    inner, outer = jnp.where(even, pair_ref[1, 0:2], pair_ref[0, 0:2]), outer_ref[0:2]
    left, right = jnp.where(even, outer, inner), jnp.where(even, inner, outer)
    message = jnp.concatenate([left, own_ref[0:2], right, jnp.zeros((2, 128), F32)], axis=0)
    message = message.astype(BF)
    for i in range(NSY):
        out_ref[i] = message


def k_bottleneck(p_ref, vt_ref, bb_ref, ow_ref, out_ref):
    p = p_ref[...].astype(F32)
    pieces = []
    none = jnp.zeros((1, 8, 128), F32)
    for a in range(3):
        moved = p if a == 0 else jnp.concatenate([p[:, a:], p[:, :a]], axis=1)
        for b in range(3):
            if b == 0:
                v = jnp.concatenate([none, moved[:-1]], axis=0)
            elif b == 1:
                v = moved
            else:
                v = jnp.concatenate([moved[1:], none], axis=0)
            pieces.append(v.reshape(128, 128).astype(BF))
    h = dot_nt(jnp.concatenate(pieces, axis=1), vt_ref[...])
    h = jnp.maximum(h + bb_ref[...], 0.0).astype(BF)
    low = dot(h, ow_ref[...])
    zero = jnp.zeros((4, 128), F32)
    rows = [zero] + [low[8 * i : 8 * i + 4] for i in range(NSY)] + [zero, zero]
    for i in range(NSY):
        out_ref[i] = jnp.concatenate(rows[i : i + 3] + [zero], axis=0).astype(BF)


def k_final(parts_ref, s_ref, w_ref, d_ref, out_ref, xt, q_ref, buf, done, sem):
    total = parts_ref[0].astype(F32)
    for i in range(1, NSY):
        total = total + parts_ref[i].astype(F32)
    total = jnp.concatenate([total, jnp.zeros((112, 128), F32)], axis=0)
    lt = jnp.transpose(total)
    lane = lanes_of(C)
    left = []
    for cell in range(4):
        here = jnp.bitwise_and(lane, 3) == cell
        left.append(jnp.concatenate([jnp.where(here, lt[:C], 0.0), jnp.where(here, lt[C:], 0.0)], axis=1).astype(BF))
    t = dot(jnp.concatenate(left, axis=0), s_ref[...])
    for cell in range(4):
        for bc in range(9):
            xt[cell, bc, pl.ds(0, C), :] = t[C * cell : C * cell + C, 128 * bc : 128 * bc + 128].astype(BF)
    products(w_ref, xt, 0, 4, into(q_ref))
    s = lax.axis_index("sx")
    first, last = s == 0, s == NSX - 1
    copies = []
    for part in range(4):
        rows = 16
        for x in range(16):
            v = d_ref[x, pl.ds(rows * part, rows), :]
            for a in range(3):
                g = x + a - 1
                num = 2 * g - 7
                low = num // 16
                high = (num - 16 * low) / 16.0
                cell = low + 1
                w_low, w_high = jnp.float32(1.0 - high), jnp.float32(high)
                if cell == 0:
                    w_low = jnp.where(first, 0.0, w_low)
                    w_high = jnp.where(first, 0.0 if g < 0 else 1.0, w_high)
                if cell == 2:
                    w_low = jnp.where(last, 0.0 if g > 15 else 1.0, w_low)
                    w_high = jnp.where(last, 0.0, w_high)
                at = pl.ds(C * a + rows * part, rows)
                v = v + w_low * q_ref[cell, at, :]
                v = v + w_high * q_ref[cell + 1, at, :]
            buf[part, pl.ds(x, rows, stride=STRIDE), :] = v
        at = pl.ds(rows * part, rows)
        for o in range(rows):
            done[rows * part + o] = buf[part, pl.ds(STRIDE * o, 16), :].astype(BF)
        copy = pltpu.make_async_copy(done.at[at], out_ref.at[at], sem.at[part])
        copy.start()
        copies.append(copy)
    for copy in copies:
        copy.wait()


def swapped(v, axis, start):
    size = lax.axis_size(axis)
    low = range(start, size - 1, 2)
    return lax.ppermute(v, axis, [(i, i + 1) for i in low] + [(i + 1, i) for i in low])


def paired(v, axis):
    pairs = [[i, i + 1] for i in range(0, lax.axis_size(axis), 2)]
    return lax.all_gather(v, axis, axis_index_groups=pairs)


def per_device(features, enc_weight, enc_bias, proj_weight, bottle_weight, bottle_bias, out_weight, dec_weight, dec_bias):
    first = (
        features,
        enc_weight.reshape(27, C, C),
        enc_bias.reshape(1, C),
        proj_weight,
        out_weight,
        bottle_bias.reshape(1, 32),
    )
    last = (dec_weight.reshape(27, C, C), dec_bias.reshape(1, C))
    ft, inner, outer, ew, eb, *deep = call(
        k_features,
        (S((18, C, 128), BF), S((2, C, 128), BF), S((2, C, 128), BF)) + tuple(S(v.shape, v.dtype) for v in first[1:]),
        *first,
        scratch=[pltpu.VMEM((C, 16, 128), BF), pltpu.VMEM((C * STRIDE, 128), F32), pltpu.SemaphoreType.DMA((6,))],
        hbm=range(6),
    )
    outer, pair = swapped(outer, "sx", 1), paired(inner, "sx")
    we, wedge, be = call(
        k_enc_weights, (S((3 * C, 9 * C), BF), S((3 * C, 6 * C), BF), S((C, 128), F32)), ew, eb, flops=10**8
    )
    xh, fl, fr, inner, outer = call(k_faces, (S((4, C, 128), BF),) + (S((5, C, 128), BF),) * 4, pair, outer, ft)
    outer, inner = swapped(outer, "sy", 1), swapped(inner, "sy", 0)
    product = call(
        k_interior,
        S((20, 3 * C + 8, 128), F32),
        ft,
        xh,
        we,
        scratch=[pltpu.VMEM((20, 9, C + 16, 128), BF)],
        flops=4 * 10**8,
    )
    em, pooled = call(k_encode, (S((18, C, 128), BF), S((8, 128), F32)), product, inner, outer, wedge, be)
    p_outer, p_pair = swapped(pooled, "sx", 1), paired(pooled, "sx")
    vt, ow2, bb2 = call(
        k_weights,
        (S((C, 9 * 128), BF), S((C, 128), BF), S((1, C), F32)),
        bottle_weight.reshape(27 * 32, 512),
        *deep,
        flops=4 * 10**8,
    )
    wd, bd, smat = call(
        k_dec_weights,
        (S((3 * C, 9 * C), BF), S((C, 128), F32), S((256, 9 * 128), BF)),
        *last,
        scratch=[pltpu.VMEM(v.shape, v.dtype) for v in last] + [pltpu.SemaphoreType.DMA((2,))],
        flops=10**8,
        hbm=(0, 1),
    )
    d = call(
        k_decode,
        S((16, C, 128), F32),
        fl,
        fr,
        inner,
        outer,
        em,
        we,
        be,
        wd,
        bd,
        scratch=[pltpu.VMEM((18, 9, C + 16, 128), BF), pltpu.VMEM((18, 3 * C + 8, 128), F32)],
        flops=4 * 10**8,
    )
    message = call(k_message, S((NSY, 8, 128), BF), p_pair, pooled, p_outer)
    everyone = lax.all_to_all(message, "sy", 0, 0, tiled=True)
    partial = call(k_bottleneck, S((NSY, 16, 128), BF), everyone, vt, bb2, ow2)
    parts = lax.all_to_all(partial, "sy", 0, 0, tiled=True)
    return call(
        k_final,
        S((C, 16, 128), BF),
        parts,
        smat,
        wd,
        d,
        scratch=[
            pltpu.VMEM((4, 9, C + 16, 128), BF),
            pltpu.VMEM((4, 3 * C + 8, 128), F32),
            pltpu.VMEM((4, 16 * STRIDE, 128), F32),
            pltpu.VMEM((C, 16, 128), BF),
            pltpu.SemaphoreType.DMA((4,)),
        ],
        out_space=pltpu.HBM,
    )


def solution(mesh):
    in_specs = (P(None, "sx", "sy"), P(), P(), P(), P(None, None, None, "sy", None), P("sy"), P("sy", None), P(), P())

    return jax.shard_map(per_device, mesh=mesh, in_specs=in_specs, out_specs=P(None, "sx", "sy"), check_vma=False)
```
